32 devices in a mesh: data: 1 (over z), pp: 4 (over y), ep: 8 (over x, core).
Axes of the slice: x: 4, y: 4, z: 1, core: 2. Of those that a mesh axis runs over, the one named last changes fastest.
The devices are a block of a 4x4x8 slice.
Arguments:
- o: bfloat16 [4, 1, 96, 768, 1792], P('pp', 'data', 'ep')
- idx: int32 [4, 1, 8, 768, 8], P('pp', 'data')
- slot: int32 [4, 1, 8, 768, 8], P('pp', 'data')
- gate: float32 [4, 1, 8, 768, 8], P('pp', 'data')
- h: bfloat16 [4, 1, 8, 768, 1792], P('pp', 'data', 'ep')
- norm_w: float32 [4, 1792], P('pp')
- wq: bfloat16 [4, 1792, 2048], P('pp')
- wk: bfloat16 [4, 1792, 2048], P('pp')
- wv: bfloat16 [4, 1792, 2048], P('pp')
- wo: bfloat16 [4, 2048, 1792], P('pp')
Outputs:
- output: bfloat16 [4, 1, 8, 768, 1792], P('pp', 'data', 'ep')
All inputs are finite; a program needn't handle non-finite values.
Results may differ from the reference program's by a relative error of at most 0.00984222.
Values are sent between devices in bfloat16 or wider.
A program may use at most 768 MiB of HBM per device.

```python
import jax
import jax.numpy as jnp
from jax import lax

PP = 4
EP = 8
M = 1
SEQ_DEV = 1
L = 768
D = 1792
E = 96
K = 8
R = 4
HEADS = 16
HEAD = 128

B = EP * SEQ_DEV
ELOC = E // EP
CAPD = 8 * ((3 * K * SEQ_DEV * L + 16 * E - 1) // (16 * E))
C = EP * CAPD
HD = HEADS * HEAD
EPS = 1e-6
SCALE = HEAD ** -0.5
WD = D ** -0.5
WH = HD ** -0.5


def route(key, dev, dev_bias, exp_bias):
    k1, k2, k3 = jax.random.split(key, 3)
    td = SEQ_DEV * L
    ds = jax.random.randint(k1, (td, EP), 0, 1 << 16) + dev_bias[None, :]
    chosen = jnp.argsort(-ds, axis=1)[:, :R]
    owner = jnp.arange(E) // ELOC
    allowed = jnp.any(owner[None, None, :] == chosen[:, :, None], axis=1)
    es = jax.random.randint(k2, (td, E), 0, 1 << 16) + exp_bias[None, :]
    es = jnp.where(allowed, es, -(1 << 30))
    ix = jnp.argsort(-es, axis=1)[:, :K].astype(jnp.int32)
    hot = (ix.reshape(td * K)[:, None] == jnp.arange(E)[None, :]).astype(jnp.int32)
    rank = jnp.sum(jnp.cumsum(hot, axis=0) * hot, axis=1) - 1
    sl = jnp.where(rank < CAPD, dev * CAPD + rank, -1).reshape(td, K).astype(jnp.int32)
    gg = 2.0 * jax.nn.softmax(1.5 * jax.random.normal(k3, (td, K), jnp.float32), axis=-1)
    return ix, sl, gg


def _route_spread(key, dev, dev_bias, exp_bias):
    lo = (K + ELOC - 1) // ELOC
    k1, k2, k3, k4, k5 = jax.random.split(key, 5)
    td = SEQ_DEV * L
    ds = jax.random.randint(k1, (td, EP), 0, 1 << 16) + dev_bias[None, :]
    rank_d = jnp.argsort(jnp.argsort(-ds, axis=1), axis=1)
    nd = jax.random.randint(k2, (td, 1), lo, R + 1)
    allowed = (rank_d < nd)[:, jnp.arange(E) // ELOC]
    es = jax.random.randint(k3, (td, E), 0, 1 << 16) + exp_bias[None, :]
    es = jnp.where(allowed, es, -(1 << 30))
    ix = jnp.argsort(-es, axis=1)[:, :K].astype(jnp.int32)
    hot = (ix.reshape(td * K)[:, None] == jnp.arange(E)[None, :]).astype(jnp.int32)
    rank = jnp.sum(jnp.cumsum(hot, axis=0) * hot, axis=1) - 1
    perm = jnp.argsort(jax.random.randint(k4, (E, CAPD), 0, 1 << 20), axis=1)
    pos = perm[ix.reshape(td * K), jnp.minimum(rank, CAPD - 1)]
    sl = jnp.where(rank < CAPD, dev * CAPD + pos, -1).reshape(td, K).astype(jnp.int32)
    gg = 2.0 * jax.nn.softmax(1.5 * jax.random.normal(k5, (td, K), jnp.float32), axis=-1)
    return ix, sl, gg


def setup_inputs(seed: int = 0, part: int = 0) -> dict:
    key = jax.random.fold_in(jax.random.key(seed), part)
    ks = jax.random.split(key, 8)
    kr = jax.random.split(jax.random.fold_in(key, 7), 3)
    dev_bias = jax.random.randint(kr[0], (EP,), 0, 1 << 15)
    exp_bias = jax.random.randint(kr[1], (E,), 0, 1 << 16)
    mu = jax.random.normal(ks[2], (PP, E, D), jnp.float32)
    sc = jax.random.uniform(ks[3], (PP, E), jnp.float32, 0.4, 1.6)

    def one_o(i):
        p = i // M
        nz = jax.random.normal(jax.random.fold_in(ks[4], i), (E, C, D), jnp.float32)
        return (sc[p][:, None, None] * (mu[p][:, None, :] + 0.5 * nz)).astype(jnp.bfloat16)

    o = lax.map(one_o, jnp.arange(PP * M)).reshape(PP, M, E, C, D)

    def one_r(i):
        return _route_spread(jax.random.fold_in(kr[2], i), i % EP, dev_bias, exp_bias)

    ix, sl, gg = lax.map(one_r, jnp.arange(PP * M * EP))
    cm = jax.random.normal(ks[6], (PP, M, B, 1, D), jnp.float32)
    nz = jax.random.normal(ks[7], (PP, M, B, L, D), jnp.float32)
    h = (0.6 * cm + 0.8 * nz).astype(jnp.bfloat16)
    kw = jax.random.split(jax.random.key(seed + 1), 5)
    norm_w = jax.random.uniform(kw[0], (PP, D), jnp.float32, 0.5, 1.5)
    wq = (1.4 * WD * jax.random.normal(kw[1], (PP, D, HD), jnp.float32)).astype(jnp.bfloat16)
    wk = (1.4 * WD * jax.random.normal(kw[2], (PP, D, HD), jnp.float32)).astype(jnp.bfloat16)
    wv = (WD * jax.random.normal(kw[3], (PP, D, HD), jnp.float32)).astype(jnp.bfloat16)
    wo = (WH * jax.random.normal(kw[4], (PP, HD, D), jnp.float32)).astype(jnp.bfloat16)
    return {'o': o, 'idx': ix.reshape(PP, M, B, L, K), 'slot': sl.reshape(PP, M, B, L, K), 'gate': gg.reshape(PP, M, B, L, K), 'h': h, 'norm_w': norm_w, 'wq': wq, 'wk': wk, 'wv': wv, 'wo': wo}


def _combine(o, ix, sl, gg, h):
    valid = sl >= 0
    rows = o.reshape(E * C, D)[jnp.where(valid, ix * C + sl, 0)].astype(jnp.float32)
    gw = jnp.where(valid, gg, 0.0)
    y = h.astype(jnp.float32) + jnp.sum(gw[..., None] * rows, axis=2)
    return y.astype(jnp.bfloat16)


def _attend(y, nw, wq, wk, wv, wo):
    yf = y.astype(jnp.float32)
    x = yf * lax.rsqrt(jnp.mean(yf * yf, axis=-1, keepdims=True) + EPS) * nw
    xb = x.astype(jnp.bfloat16).reshape(B * L, D)
    q = jnp.dot(xb, wq, preferred_element_type=jnp.float32).astype(jnp.bfloat16).reshape(B, L, HEADS, HEAD)
    kt = jnp.dot(xb, wk, preferred_element_type=jnp.float32).astype(jnp.bfloat16).reshape(B, L, HEADS, HEAD)
    vt = jnp.dot(xb, wv, preferred_element_type=jnp.float32).astype(jnp.bfloat16).reshape(B, L, HEADS, HEAD)
    causal = jnp.arange(L)[:, None] >= jnp.arange(L)[None, :]

    def one(a):
        s = jnp.einsum('qhd,khd->hqk', a[0].astype(jnp.float32), a[1].astype(jnp.float32)) * SCALE
        pr = jax.nn.softmax(jnp.where(causal[None], s, -1e30), axis=-1).astype(jnp.bfloat16)
        return jnp.einsum('hqk,khd->qhd', pr.astype(jnp.float32), a[2].astype(jnp.float32)).astype(jnp.bfloat16)

    att = lax.map(one, (q, kt, vt)).reshape(B * L, HD)
    out = jnp.dot(att, wo, preferred_element_type=jnp.float32).astype(jnp.bfloat16).reshape(B, L, D)
    return (yf + out.astype(jnp.float32)).astype(jnp.bfloat16)


def reference(o, idx, slot, gate, h, norm_w, wq, wk, wv, wo):
    y = lax.map(lambda a: _combine(a[0], a[1], a[2], a[3], a[4]), (o.reshape(PP * M, E, C, D), idx.reshape(PP * M, B, L, K), slot.reshape(PP * M, B, L, K), gate.reshape(PP * M, B, L, K), h.reshape(PP * M, B, L, D)))
    yin = jnp.roll(y.reshape(PP, M, B, L, D), 1, axis=0).reshape(PP * M, B, L, D)
    stage = jnp.arange(PP * M) // M
    z = lax.map(lambda a: _attend(a[0], norm_w[a[1]], wq[a[1]], wk[a[1]], wv[a[1]], wo[a[1]]), (yin, stage))
    return z.reshape(PP, M, B, L, D)
```

```python
import jax
import jax.numpy as jnp
from jax import lax
from jax.experimental import pallas as pl
from jax.experimental.pallas import tpu as pltpu
from jax.sharding import PartitionSpec as P

HEAD = 128
EPS = 1e-6
SCALE = HEAD ** -0.5
MESH = pl.DeviceIdType.MESH
F32 = jnp.float32
BF16 = jnp.bfloat16
DPOS = (2, 1, 3, 0)
HALF = 64
NS = 3
NP = 2


def attend(y, nw, wq, wk, wv, wo):
    nm, ns, ln, d = y.shape
    hd = wq.shape[1]
    nh = hd // HEAD
    yf = y.astype(jnp.float32)
    x = yf * lax.rsqrt(jnp.mean(yf * yf, axis=-1, keepdims=True) + EPS) * nw
    xb = x.astype(jnp.bfloat16)
    shp = (nm, ns, ln, nh, HEAD)
    q = jnp.einsum('msld,de->msle', xb, wq, preferred_element_type=jnp.float32).astype(jnp.bfloat16).reshape(shp)
    kt = jnp.einsum('msld,de->msle', xb, wk, preferred_element_type=jnp.float32).astype(jnp.bfloat16).reshape(shp)
    vt = jnp.einsum('msld,de->msle', xb, wv, preferred_element_type=jnp.float32).astype(jnp.bfloat16).reshape(shp)
    sc = jnp.einsum('msqhd,mskhd->mshqk', q, kt, preferred_element_type=jnp.float32) * SCALE
    causal = lax.broadcasted_iota(jnp.int32, (ln, ln), 0) >= lax.broadcasted_iota(jnp.int32, (ln, ln), 1)
    pr = jax.nn.softmax(jnp.where(causal, sc, -1e30), axis=-1).astype(jnp.bfloat16)
    att = jnp.einsum('mshqk,mskhd->msqhd', pr, vt, preferred_element_type=jnp.float32).astype(jnp.bfloat16).reshape(nm, ns, ln, hd)
    out = jnp.einsum('msle,ed->msld', att, wo, preferred_element_type=jnp.float32).astype(jnp.bfloat16)
    return (yf + out.astype(jnp.float32)).astype(jnp.bfloat16)


def make_combine(n, npp, el, c, d, ln, kk):
    nx = n // 2
    assert nx == 4
    capd = c // n
    ec = 2 * el
    kd = ec * capd
    tt = 2 * HALF
    npair = ln // tt
    nu = 4 * npair
    pw = d // NP
    half = HALF

    def kernel(o, idx, slot, gate, h, yin, ox, pan, gm, pb, h1, fin, ib, sb, gb, hb, yb,
               xs, xr, h1s, h1r, pls, plr, cbs, cbr, ys, yr, psem, isem, hsem):
        ep = lax.axis_index('ep')
        pp = lax.axis_index('pp')
        core = lax.rem(ep, 2)
        x = ep // 2
        partner = {'ep': 2 * x + 1 - core}
        right = {'ep': 2 * lax.rem(x + 1, nx) + core}
        left = {'ep': 2 * lax.rem(x + nx - 1, nx) + core}
        ynext = {'pp': lax.rem(pp + 1, npp)}
        yprev = {'pp': lax.rem(pp + npp - 1, npp)}

        bar = pltpu.get_barrier_semaphore()
        for dev in (partner, right, left, ynext, yprev):
            pl.semaphore_signal(bar, inc=1, device_id=dev, device_id_type=MESH)
        pl.semaphore_wait(bar, 5)

        def remote(src, dst, ss, rs, dev):
            return pltpu.make_async_remote_copy(src_ref=src, dst_ref=dst, send_sem=ss, recv_sem=rs, device_id=dev, device_id_type=MESH)

        def owner(dp, cc):
            dd = jnp.where(dp == 0, 2, jnp.where(dp == 1, 1, jnp.where(dp == 2, 3, 0)))
            return 2 * lax.rem(x + dd, nx) + cc

        def exch(dp):
            q = owner(dp, 1 - core)
            src = o.at[:, pl.ds(pl.multiple_of(q * capd, capd), capd), :]
            return remote(src, ox.at[dp], xs.at[dp], xr.at[dp], partner)

        def small(u):
            i = u // 4
            q = owner(lax.rem(u, 4), core)
            b = lax.rem(u, 2)
            rows = pl.ds(pl.multiple_of(i * tt, tt), tt)
            return [pltpu.make_async_copy(a.at[q, rows, :], v.at[b], isem.at[b, k])
                    for k, (a, v) in enumerate(((idx, ib), (slot, sb), (gate, gb)))]

        def panel(s):
            u = s // NP
            dp = lax.rem(u, 4)
            q = owner(dp, core)
            b = lax.rem(s, NS)
            cols = pl.ds(pl.multiple_of(lax.rem(s, NP) * pw, pw), pw)
            own = pltpu.make_async_copy(o.at[:, pl.ds(pl.multiple_of(q * capd, capd), capd), cols],
                                        pan.at[b, pl.ds(core * el, el)], psem.at[b, 0])
            oth = pltpu.make_async_copy(ox.at[dp, :, :, cols], pan.at[b, pl.ds((1 - core) * el, el)], psem.at[b, 1])
            return own, oth

        def hop(i, way):
            dev = right if way == 0 else left
            src = pb.at[4 * lax.rem(i, 2), pl.ds(way * half, half), :]
            return remote(src, h1.at[way, i], h1s.at[way, i], h1r.at[way, i], dev)

        def plain(i, way):
            dev = right if way == 0 else left
            at = pl.ds((1 - way) * half, half)
            src = pb.at[4 * lax.rem(i, 2) + 1 + way, at, :]
            return remote(src, fin.at[way, i, at, :], pls.at[way, i], plr.at[way, i], dev)

        def comb(i, way):
            dev = right if way == 0 else left
            at = pl.ds(way * half, half)
            src = pb.at[4 * lax.rem(i, 2) + 1 + way, at, :]
            return remote(src, fin.at[way, i, at, :], cbs.at[way, i], cbr.at[way, i], dev)

        def hload(i):
            b = lax.rem(i, 2)
            return pltpu.make_async_copy(h.at[pl.ds(pl.multiple_of(i * tt, tt), tt), :], hb.at[b], hsem.at[b])

        def ysend(i):
            rows = pl.ds(pl.multiple_of(i * tt, tt), tt)
            return remote(yb.at[lax.rem(i, 2)], yin.at[rows, :], ys.at[i], yr.at[i], ynext)

        def gates(u, g0, g1):
            b = lax.rem(u, 2)
            q = owner(lax.rem(u, 4), core)
            lo_e = x * ec
            for g in range(g0, g1):
                rows = pl.ds(16 * g, 16)
                ii, ss, gg = ib[b, rows, :], sb[b, rows, :], gb[b, rows, :]
                e = ii - lo_e
                ok = (e >= 0) & (e < ec) & (ss >= 0)
                col = jnp.where(ok, e * capd + (ss - q * capd), -1)
                cs = [jnp.broadcast_to(col[:, j:j + 1], (16, 128)) for j in range(kk)]
                ws = [jnp.broadcast_to(gg[:, j:j + 1], (16, 128)) for j in range(kk)]
                io = lax.broadcasted_iota(jnp.int32, (16, 128), 1)
                for v in range(kd // 128):
                    at = io + 128 * v
                    t = jnp.zeros((16, 128), F32)
                    for j in range(kk):
                        t = jnp.where(cs[j] == at, ws[j], t)
                    hi = t.astype(BF16)
                    r = t - hi.astype(F32)
                    mi = r.astype(BF16)
                    lw = (r - mi.astype(F32)).astype(BF16)
                    for k, part in enumerate((hi, mi, lw)):
                        gm[b, pl.ds(k * tt + 16 * g, 16), 128 * v:128 * v + 128] = part

        def finish(i):
            for way in range(2):
                plain(i, way).wait_recv()
                comb(i, way).wait_recv()
            hload(i).wait()
            b = lax.rem(i, 2)

            @pl.when(i >= 2)
            def _():
                ysend(i - 2).wait_send()

            def rows16(r, _):
                at = pl.ds(pl.multiple_of(r * 16, 16), 16)
                y = hb[b, at, :].astype(F32) + (pb[4 * b + 3, at, :] + (fin[0, i, at, :] + fin[1, i, at, :]))
                yb[b, at, :] = y.astype(BF16)
                return 0

            lax.fori_loop(0, tt // 16, rows16, 0)
            ysend(i).start()

        for dp in range(4):
            exch(dp).start()
        for cp in small(0) + small(1):
            cp.start()
        hload(0).start()
        for cp in small(0):
            cp.wait()
        gates(0, 0, tt // 16)
        exch(0).wait_recv()
        for s in range(NS - 1):
            for cp in panel(s):
                cp.start()

        def unit(u, _):
            i = u // 4
            dp = lax.rem(u, 4)
            b = lax.rem(u, 2)
            par = lax.rem(i, 2)
            dst = 4 * par + dp

            @pl.when(u + 1 < nu)
            def _():
                for cp in small(u + 1):
                    cp.wait()

            @pl.when((i >= 2) & (dp == 0))
            def _():
                for way in range(2):
                    hop(i - 2, way).wait_send()
                    plain(i - 2, way).wait_send()
                    comb(i - 2, way).wait_send()

            def step(k, _):
                s = NP * u + k
                nxt = s + NS - 1

                @pl.when((nxt < 4 * NP) & (lax.rem(nxt, NP) == 0))
                def _():
                    exch(nxt // NP).wait_recv()

                @pl.when(nxt < nu * NP)
                def _():
                    for cp in panel(nxt):
                        cp.start()

                for cp in panel(s):
                    cp.wait()
                w = pan[lax.rem(s, NS)].reshape(kd, pw)
                acc = jnp.dot(gm[b], w, preferred_element_type=F32)
                res = acc[0:tt] + (acc[tt:2 * tt] + acc[2 * tt:3 * tt])
                pb[dst, :, pl.ds(pl.multiple_of(k * pw, pw), pw)] = res
                return 0

            lax.fori_loop(0, NP, step, 0)
            gates(u + 1, 0, tt // 16)

            @pl.when(u + 2 < nu)
            def _():
                for cp in small(u + 2):
                    cp.start()

            @pl.when(dp == 0)
            def _():
                hop(i, 0).start()
                hop(i, 1).start()

            @pl.when(dp == 1)
            def _():
                plain(i, 0).start()

            @pl.when(dp == 2)
            def _():
                plain(i, 1).start()

            @pl.when(dp == 3)
            def _():
                for way in range(2):
                    hop(i, way).wait_recv()
                    src = 4 * par + 1 + way

                    def add(r, _, way=way, src=src):
                        at = pl.ds(pl.multiple_of(way * half + r * 16, 16), 16)
                        pb[src, at, :] = pb[src, at, :] + h1[way, i, pl.ds(pl.multiple_of(r * 16, 16), 16), :]
                        return 0

                    lax.fori_loop(0, half // 16, add, 0)
                    comb(i, way).start()

                @pl.when(i >= 1)
                def _():
                    finish(i - 1)

                @pl.when(i + 1 < npair)
                def _():
                    hload(i + 1).start()
            return 0

        lax.fori_loop(0, nu, unit, 0)
        finish(npair - 1)
        for dp in range(4):
            exch(dp).wait_send()
        for i in range(max(npair - 2, 0), npair):
            for way in range(2):
                hop(i, way).wait_send()
                plain(i, way).wait_send()
                comb(i, way).wait_send()
            ysend(i).wait_send()
        for i in range(npair):
            ysend(i).wait_recv()

    dma = pltpu.SemaphoreType.DMA
    anyspec = pl.BlockSpec(memory_space=pl.ANY)
    flops = 2 * 3 * 4 * ln * kd * d
    return pl.pallas_call(
        kernel,
        out_shape=(jax.ShapeDtypeStruct((ln, d), BF16), jax.ShapeDtypeStruct((4, el, capd, d), BF16)),
        in_specs=[anyspec] * 5,
        out_specs=(anyspec, anyspec),
        scratch_shapes=[
            pltpu.VMEM((NS, ec, capd, pw), BF16),
            pltpu.VMEM((2, 3 * tt, kd), BF16),
            pltpu.VMEM((8, tt, d), F32),
            pltpu.VMEM((2, npair, half, d), F32),
            pltpu.VMEM((2, npair, tt, d), F32),
            pltpu.VMEM((2, tt, kk), jnp.int32),
            pltpu.VMEM((2, tt, kk), jnp.int32),
            pltpu.VMEM((2, tt, kk), F32),
            pltpu.VMEM((2, tt, d), BF16),
            pltpu.VMEM((2, tt, d), BF16),
            dma((4,)), dma((4,)),
            dma((2, npair)), dma((2, npair)), dma((2, npair)), dma((2, npair)), dma((2, npair)), dma((2, npair)),
            dma((npair,)), dma((npair,)),
            dma((NS, 2)), dma((2, 3)), dma((2,)),
        ],
        compiler_params=pltpu.CompilerParams(collective_id=1, has_side_effects=True, vmem_limit_bytes=60 << 20),
        cost_estimate=pl.CostEstimate(flops=flops, bytes_accessed=200 << 20, transcendentals=0),
        name='combine',
    )


def solution(mesh):
    n = mesh.shape['ep']
    npp = mesh.shape['pp']
    sp_o = P('pp', 'data', 'ep', None, None)
    sp_r = P('pp', 'data', None, None, None)
    sp_1 = P('pp', None)
    sp_w = P('pp', None, None)

    def body(o, idx, slot, gate, h, norm_w, wq, wk, wv, wo):
        _, nm, el, c, d = o.shape
        ln, kk = h.shape[3], idx.shape[4]
        assert nm == 1 and h.shape[2] == 1
        combine = make_combine(n, npp, el, c, d, ln, kk)
        yin, _ = combine(o.reshape(el, c, d), idx.reshape(n, ln, kk), slot.reshape(n, ln, kk), gate.reshape(n, ln, kk), h.reshape(ln, d))
        z = attend(yin.reshape(1, 1, ln, d), norm_w[0], wq[0], wk[0], wv[0], wo[0])
        return z[None]

    return jax.shard_map(body, mesh=mesh, in_specs=(sp_o, sp_r, sp_r, sp_r, sp_o, sp_1, sp_w, sp_w, sp_w, sp_w), out_specs=sp_o, check_vma=False)
```

```python
import jax
import jax.numpy as jnp
from jax import lax
from jax.experimental import pallas as pl
from jax.experimental.pallas import tpu as pltpu
from jax.sharding import PartitionSpec as P

HEAD = 128
EPS = 1e-6
SCALE = HEAD ** -0.5
MESH = pl.DeviceIdType.MESH
F32 = jnp.float32
BF16 = jnp.bfloat16
HALF = 64
NS = 3
NP = 2
NW = 3
WQ = 512
WZ = 256


def make_stage(n, npp, el, c, d, ln, kk, hd):
    nx = n // 2
    assert nx == 4
    capd = c // n
    ec = 2 * el
    kd = ec * capd
    tt = 2 * HALF
    npair = ln // tt
    nu = 4 * npair
    pw = d // NP
    half = HALF
    nq = hd // WQ
    nz = d // WZ
    nwp = 3 * nq + nz
    nh = hd // HEAD

    def kernel(o, idx, slot, gate, h, nw, wq, wk, wv, wo, z, ox,
               pan, gm0, gm1, colt, gatet, pb, h1, fin, ib, sb, gb, hb, yb, yv, xb, wb, qb, kv, ab, zb,
               xs, xr, h1s, h1r, pls, plr, cbs, cbr, ys, yr, psem, isem, hsem, wsem, zsem):
        ep = lax.axis_index('ep')
        pp = lax.axis_index('pp')
        core = lax.rem(ep, 2)
        x = ep // 2
        partner = {'ep': 2 * x + 1 - core}
        right = {'ep': 2 * lax.rem(x + 1, nx) + core}
        left = {'ep': 2 * lax.rem(x + nx - 1, nx) + core}
        ynext = {'pp': lax.rem(pp + 1, npp)}
        yprev = {'pp': lax.rem(pp + npp - 1, npp)}

        def remote(src, dst, ss, rs, dev):
            return pltpu.make_async_remote_copy(src_ref=src, dst_ref=dst, send_sem=ss, recv_sem=rs, device_id=dev, device_id_type=MESH)

        def owner(dp, cc):
            dd = jnp.where(dp == 0, 2, jnp.where(dp == 1, 1, jnp.where(dp == 2, 3, 0)))
            return 2 * lax.rem(x + dd, nx) + cc

        def exch(dp):
            q = owner(dp, 1 - core)
            src = o.at[:, pl.ds(pl.multiple_of(q * capd, capd), capd), :]
            return remote(src, ox.at[dp], xs.at[dp], xr.at[dp], partner)

        def small(u):
            i = u // 4
            q = owner(lax.rem(u, 4), core)
            b = lax.rem(u, 2)
            cols = pl.ds(pl.multiple_of(i * tt, tt), tt)
            return [pltpu.make_async_copy(a.at[q, :, cols], v.at[b], isem.at[b, k])
                    for k, (a, v) in enumerate(((idx, ib), (slot, sb), (gate, gb)))]

        def panel(s):
            u = s // NP
            dp = lax.rem(u, 4)
            q = owner(dp, core)
            b = lax.rem(s, NS)
            cols = pl.ds(pl.multiple_of(lax.rem(s, NP) * pw, pw), pw)
            own = pltpu.make_async_copy(o.at[:, pl.ds(pl.multiple_of(q * capd, capd), capd), cols],
                                        pan.at[b, pl.ds(core * el, el)], psem.at[b, 0])
            oth = pltpu.make_async_copy(ox.at[dp, :, :, cols], pan.at[b, pl.ds((1 - core) * el, el)], psem.at[b, 1])
            return own, oth

        def hop(i, way):
            dev = right if way == 0 else left
            src = pb.at[4 * lax.rem(i, 2), pl.ds(way * half, half), :]
            return remote(src, h1.at[way, i], h1s.at[way, i], h1r.at[way, i], dev)

        def plain(i, way):
            dev = right if way == 0 else left
            at = pl.ds((1 - way) * half, half)
            src = pb.at[4 * lax.rem(i, 2) + 1 + way, at, :]
            return remote(src, fin.at[way, i, at, :], pls.at[way, i], plr.at[way, i], dev)

        def comb(i, way):
            dev = right if way == 0 else left
            at = pl.ds(way * half, half)
            src = pb.at[4 * lax.rem(i, 2) + 1 + way, at, :]
            return remote(src, fin.at[way, i, at, :], cbs.at[way, i], cbr.at[way, i], dev)

        def hload(i):
            b = lax.rem(i, 2)
            return pltpu.make_async_copy(h.at[pl.ds(pl.multiple_of(i * tt, tt), tt), :], hb.at[b], hsem.at[b])

        def ysend(i):
            rows = pl.ds(pl.multiple_of(i * tt, tt), tt)
            return remote(yb.at[lax.rem(i, 2)], yv.at[rows, :], ys.at[i], yr.at[i], ynext)

        def wcopy(which, k, t):
            b = lax.rem(t, NW)
            if which < 3:
                src = (wq, wk, wv)[which].at[:, pl.ds(pl.multiple_of(k * WQ, WQ), WQ)]
                return pltpu.make_async_copy(src, wb.at[b, pl.ds(0, d), :], wsem.at[b])
            src = wo.at[:, pl.ds(pl.multiple_of(k * WZ, WZ), WZ)]
            return pltpu.make_async_copy(src, wb.at[b, :, pl.ds(0, WZ)], wsem.at[b])

        def wstart(t):
            r = lax.rem(t, nwp)

            @pl.when(t < nwp * npair)
            def _():
                for which in range(3):
                    @pl.when((r >= which * nq) & (r < (which + 1) * nq))
                    def _(which=which):
                        wcopy(which, r - which * nq, t).start()

                @pl.when(r >= 3 * nq)
                def _():
                    wcopy(3, r - 3 * nq, t).start()

        def zcopy(j):
            b = lax.rem(j, 2)
            return pltpu.make_async_copy(zb.at[b], z.at[pl.ds(pl.multiple_of(j * tt, tt), tt), :], zsem.at[b])

        def columns(u, b):
            q = owner(lax.rem(u, 4), core)
            e = ib[b] - x * ec
            ss = sb[b]
            ok = (e >= 0) & (e < ec) & (ss >= 0)
            col = jnp.where(ok, e * capd + (ss - q * capd), -1)
            colt[...] = col.T
            gatet[...] = gb[b].T

        def gates(gm, g0, g1):
            for g in range(g0, g1):
                rows = pl.ds(16 * g, 16)
                col = colt[rows, :].astype(jnp.int16)
                gg = gatet[rows, :]
                hi = gg.astype(BF16)
                r = gg - hi.astype(F32)
                mi = r.astype(BF16)
                lw = (r - mi.astype(F32)).astype(BF16)
                cs = [jnp.broadcast_to(col[:, j:j + 1], (16, 128)) for j in range(kk)]
                ws = [[jnp.broadcast_to(p[:, j:j + 1], (16, 128)) for j in range(kk)] for p in (hi, mi, lw)]
                io = lax.broadcasted_iota(jnp.int16, (16, 128), 1)
                for v in range(kd // 128):
                    at = io + jnp.int16(128 * v)
                    t = [jnp.zeros((16, 128), BF16) for _ in range(3)]
                    for j in range(kk):
                        m = cs[j] == at
                        for k in range(3):
                            t[k] = jnp.where(m, ws[k][j], t[k])
                    for k in range(3):
                        gm[k * tt + 16 * g:k * tt + 16 * g + 16, 128 * v:128 * v + 128] = t[k]

        def finish(i):
            for way in range(2):
                plain(i, way).wait_recv()
                comb(i, way).wait_recv()
            hload(i).wait()
            b = lax.rem(i, 2)

            @pl.when(i >= 2)
            def _():
                ysend(i - 2).wait_send()

            def rows16(r, _):
                at = pl.ds(pl.multiple_of(r * 16, 16), 16)
                y = hb[b, at, :].astype(F32) + (pb[4 * b + 3, at, :] + (fin[0, i, at, :] + fin[1, i, at, :]))
                yb[b, at, :] = y.astype(BF16)
                return 0

            lax.fori_loop(0, tt // 16, rows16, 0)
            ysend(i).start()

        def attend(j):
            ysend(j).wait_recv()
            base = pl.multiple_of(j * tt, tt)
            t0 = nwp * j

            def norm(r, _):
                at = pl.ds(pl.multiple_of(r * 16, 16), 16)
                y = yv[pl.ds(pl.multiple_of(base + r * 16, 16), 16), :].astype(F32)
                xf = y * lax.rsqrt(jnp.mean(y * y, axis=-1, keepdims=True) + EPS) * nw[...]
                xb[at, :] = xf.astype(BF16)
                return 0

            lax.fori_loop(0, tt // 16, norm, 0)

            def project(k, _):
                t = t0 + k
                wcopy(0, 0, t).wait()
                r = jnp.dot(xb[...], wb[lax.rem(t, NW), 0:d, :], preferred_element_type=F32).astype(BF16)
                cols = pl.ds(pl.multiple_of(lax.rem(k, nq) * WQ, WQ), WQ)

                @pl.when(k < nq)
                def _():
                    qb[:, cols] = r

                @pl.when(k >= nq)
                def _():
                    kv[k // nq - 1, pl.ds(base, tt), cols] = r

                wstart(t + NW)
                return 0

            lax.fori_loop(0, 3 * nq, project, 0)

            for jj in range(npair):
                @pl.when(j == jj)
                def _(jj=jj):
                    nk = tt * (jj + 1)

                    def heads(g, _):
                        for a in range(2):
                            cols = pl.ds(pl.multiple_of((2 * g + a) * HEAD, HEAD), HEAD)
                            s = lax.dot_general(qb[:, cols], kv[0, 0:nk, cols], (((1,), (1,)), ((), ())), preferred_element_type=F32) * SCALE
                            row = lax.broadcasted_iota(jnp.int32, (tt, nk), 0) + tt * jj
                            s = jnp.where(row >= lax.broadcasted_iota(jnp.int32, (tt, nk), 1), s, -1e30)
                            p = jnp.exp(s - jnp.max(s, axis=-1, keepdims=True))
                            p = (p * (1.0 / jnp.sum(p, axis=-1, keepdims=True))).astype(BF16)
                            ab[:, cols] = jnp.dot(p, kv[1, 0:nk, cols], preferred_element_type=F32).astype(BF16)
                        return 0

                    lax.fori_loop(0, nh // 2, heads, 0)

            b = lax.rem(j, 2)

            @pl.when(j >= 2)
            def _():
                zcopy(j - 2).wait()

            def out(k, _):
                t = t0 + 3 * nq + k
                wcopy(3, 0, t).wait()
                r = jnp.dot(ab[...], wb[lax.rem(t, NW), :, 0:WZ], preferred_element_type=F32).astype(BF16)
                cols = pl.ds(pl.multiple_of(k * WZ, WZ), WZ)
                zb[b, :, cols] = (yv[pl.ds(base, tt), cols].astype(F32) + r.astype(F32)).astype(BF16)
                wstart(t + NW)
                return 0

            lax.fori_loop(0, nz, out, 0)
            zcopy(j).start()

        def unit(i, dp, gmc, gmn, bn):
            u = 4 * i + dp
            dst = 4 * lax.rem(i, 2) + dp

            @pl.when(u + 1 < nu)
            def _():
                for cp in small(u + 1):
                    cp.wait()

            columns(u + 1, bn)

            @pl.when(u + 3 < nu)
            def _():
                for cp in small(u + 3):
                    cp.start()

            ng = tt // 16 // NP
            for k in range(NP):
                s = NP * u + k
                nxt = s + NS - 1

                @pl.when((nxt < 4 * NP) & (lax.rem(nxt, NP) == 0))
                def _(nxt=nxt):
                    exch(nxt // NP).wait_recv()

                @pl.when(nxt < nu * NP)
                def _(nxt=nxt):
                    for cp in panel(nxt):
                        cp.start()

                for cp in panel(s):
                    cp.wait()
                w = pan[lax.rem(s, NS)].reshape(kd, pw)
                acc = jnp.dot(gmc[...], w, preferred_element_type=F32)
                pb[dst, :, k * pw:(k + 1) * pw] = acc[0:tt] + (acc[tt:2 * tt] + acc[2 * tt:3 * tt])
                gates(gmn, ng * k, ng * (k + 1))

        bar = pltpu.get_barrier_semaphore()
        for dev in (partner, right, left, ynext, yprev):
            pl.semaphore_signal(bar, inc=1, device_id=dev, device_id_type=MESH)
        pl.semaphore_wait(bar, 5)

        for dp in range(4):
            exch(dp).start()
        for u in range(2):
            for cp in small(u):
                cp.start()
        for t in range(NW):
            wstart(jnp.int32(t))
        for cp in small(0):
            cp.wait()
        columns(jnp.int32(0), 0)
        for cp in small(2):
            cp.start()
        hload(0).start()
        gates(gm0, 0, tt // 16)
        exch(0).wait_recv()
        for s in range(NS - 1):
            for cp in panel(s):
                cp.start()

        def iteration(i, _):
            @pl.when(i < npair)
            def _():
                @pl.when(i >= 2)
                def _():
                    for way in range(2):
                        hop(i - 2, way).wait_send()
                        plain(i - 2, way).wait_send()
                        comb(i - 2, way).wait_send()

                def two(v, _):
                    unit(i, 2 * v, gm0, gm1, 1)

                    @pl.when(v == 0)
                    def _():
                        hop(i, 0).start()
                        hop(i, 1).start()

                    @pl.when(v == 1)
                    def _():
                        plain(i, 1).start()

                    unit(i, 2 * v + 1, gm1, gm0, 0)

                    @pl.when(v == 0)
                    def _():
                        plain(i, 0).start()
                    return 0

                lax.fori_loop(0, 2, two, 0)
                for way in range(2):
                    hop(i, way).wait_recv()
                    src = 4 * lax.rem(i, 2) + 1 + way

                    def add(r, _, way=way, src=src):
                        at = pl.ds(pl.multiple_of(way * half + r * 16, 16), 16)
                        pb[src, at, :] = pb[src, at, :] + h1[way, i, pl.ds(pl.multiple_of(r * 16, 16), 16), :]
                        return 0

                    lax.fori_loop(0, half // 16, add, 0)
                    comb(i, way).start()

            @pl.when((i >= 1) & (i <= npair))
            def _():
                finish(i - 1)

            @pl.when(i + 1 < npair)
            def _():
                hload(i + 1).start()

            @pl.when(i >= 2)
            def _():
                attend(i - 2)
            return 0

        lax.fori_loop(0, npair + 2, iteration, 0)
        for dp in range(4):
            exch(dp).wait_send()
        for i in range(max(npair - 2, 0), npair):
            for way in range(2):
                hop(i, way).wait_send()
                plain(i, way).wait_send()
                comb(i, way).wait_send()
            ysend(i).wait_send()
            zcopy(i).wait()

    dma = pltpu.SemaphoreType.DMA
    anyspec = pl.BlockSpec(memory_space=pl.ANY)
    flops = 2 * 3 * 4 * ln * kd * d
    return pl.pallas_call(
        kernel,
        out_shape=(jax.ShapeDtypeStruct((ln, d), BF16), jax.ShapeDtypeStruct((4, el, capd, d), BF16)),
        in_specs=[anyspec] * 5 + [pl.BlockSpec(memory_space=pltpu.VMEM)] + [anyspec] * 4,
        out_specs=(anyspec, anyspec),
        scratch_shapes=[
            pltpu.VMEM((NS, ec, capd, pw), BF16),
            pltpu.VMEM((3 * tt, kd), BF16),
            pltpu.VMEM((3 * tt, kd), BF16),
            pltpu.VMEM((tt, kk), jnp.int32),
            pltpu.VMEM((tt, kk), F32),
            pltpu.VMEM((8, tt, d), F32),
            pltpu.VMEM((2, npair, half, d), F32),
            pltpu.VMEM((2, npair, tt, d), F32),
            pltpu.VMEM((2, kk, tt), jnp.int32),
            pltpu.VMEM((2, kk, tt), jnp.int32),
            pltpu.VMEM((2, kk, tt), F32),
            pltpu.VMEM((2, tt, d), BF16),
            pltpu.VMEM((2, tt, d), BF16),
            pltpu.VMEM((ln, d), BF16),
            pltpu.VMEM((tt, d), BF16),
            pltpu.VMEM((NW, hd, WQ), BF16),
            pltpu.VMEM((tt, hd), BF16),
            pltpu.VMEM((2, ln, hd), BF16),
            pltpu.VMEM((tt, hd), BF16),
            pltpu.VMEM((2, tt, d), BF16),
            dma((4,)), dma((4,)),
            dma((2, npair)), dma((2, npair)), dma((2, npair)), dma((2, npair)), dma((2, npair)), dma((2, npair)),
            dma((npair,)), dma((npair,)),
            dma((NS, 2)), dma((2, 3)), dma((2,)), dma((NW,)), dma((2,)),
        ],
        compiler_params=pltpu.CompilerParams(collective_id=1, has_side_effects=True, vmem_limit_bytes=67043328),
        cost_estimate=pl.CostEstimate(flops=flops, bytes_accessed=200 << 20, transcendentals=0),
        name='stage',
    )


def solution(mesh):
    n = mesh.shape['ep']
    npp = mesh.shape['pp']
    sp_o = P('pp', 'data', 'ep', None, None)
    sp_r = P('pp', 'data', None, None, None)
    sp_1 = P('pp', None)
    sp_w = P('pp', None, None)

    def body(o, idx, slot, gate, h, norm_w, wq, wk, wv, wo):
        _, nm, el, c, d = o.shape
        ln, kk = h.shape[3], idx.shape[4]
        hd = wq.shape[2]
        assert nm == 1 and h.shape[2] == 1
        stage = make_stage(n, npp, el, c, d, ln, kk, hd)
        turn = [jnp.swapaxes(a.reshape(n, ln, kk), 1, 2) for a in (idx, slot, gate)]
        z, _ = stage(o.reshape(el, c, d), *turn, h.reshape(ln, d), norm_w, wq[0], wk[0], wv[0], wo[0])
        return z.reshape(h.shape)

    return jax.shard_map(body, mesh=mesh, in_specs=(sp_o, sp_r, sp_r, sp_r, sp_o, sp_1, sp_w, sp_w, sp_w, sp_w), out_specs=sp_o, check_vma=False)
```

```python
import jax
import jax.numpy as jnp
from jax import lax
from jax.experimental import pallas as pl
from jax.experimental.pallas import tpu as pltpu
from jax.sharding import PartitionSpec as P

HEAD = 128
EPS = 1e-6
SCALE2 = HEAD ** -0.5 * 1.4426950408889634
MESH = pl.DeviceIdType.MESH
F32 = jnp.float32
BF16 = jnp.bfloat16
HALF = 64
NS = 3
NP = 2
NW = 3
NB = 4
GROUPS = ((0, 2), (2, 2), (4, 1), (5, 1))
WQ = 512
WZ = 256


def make_stage(n, npp, el, c, d, ln, kk, hd):
    nx = n // 2
    assert nx == 4
    capd = c // n
    ec = 2 * el
    kd = ec * capd
    tt = 2 * HALF
    npair = ln // tt
    nu = 4 * npair
    pw = d // NP
    half = HALF
    nq = hd // WQ
    nz = d // WZ
    nwp = 3 * nq + nz
    nh = hd // HEAD
    mg = tt * max(count for _, count in GROUPS)
    assert sum(count for _, count in GROUPS) == npair

    def kernel(o, idx, slot, gate, h, nw, wq, wk, wv, wo, z, ox,
               pan, gm0, gm1, colt, gatet, pb, h1, fin, ib, sb, gb, hb, yb, yv, xb, wb, qb, kv, ab, zb,
               xs, xr, h1s, h1r, pls, plr, cbs, cbr, ys, yr, psem, isem, hsem, wsem, zsem):
        ep = lax.axis_index('ep')
        pp = lax.axis_index('pp')
        core = lax.rem(ep, 2)
        x = ep // 2
        partner = {'ep': 2 * x + 1 - core}
        right = {'ep': 2 * lax.rem(x + 1, nx) + core}
        left = {'ep': 2 * lax.rem(x + nx - 1, nx) + core}
        ynext = {'pp': lax.rem(pp + 1, npp)}
        yprev = {'pp': lax.rem(pp + npp - 1, npp)}

        def remote(src, dst, ss, rs, dev):
            return pltpu.make_async_remote_copy(src_ref=src, dst_ref=dst, send_sem=ss, recv_sem=rs, device_id=dev, device_id_type=MESH)

        def owner(dp, cc):
            dd = jnp.where(dp == 0, 2, jnp.where(dp == 1, 1, jnp.where(dp == 2, 3, 0)))
            return 2 * lax.rem(x + dd, nx) + cc

        def exch(dp):
            q = owner(dp, 1 - core)
            src = o.at[:, pl.ds(pl.multiple_of(q * capd, capd), capd), :]
            return remote(src, ox.at[dp], xs.at[dp], xr.at[dp], partner)

        def small(u):
            i = u // 4
            q = owner(lax.rem(u, 4), core)
            b = lax.rem(u, 2)
            cols = pl.ds(pl.multiple_of(i * tt, tt), tt)
            return [pltpu.make_async_copy(a.at[q, :, cols], v.at[b], isem.at[b, k])
                    for k, (a, v) in enumerate(((idx, ib), (slot, sb), (gate, gb)))]

        def panel(s):
            u = s // NP
            dp = lax.rem(u, 4)
            q = owner(dp, core)
            b = lax.rem(s, NS)
            cols = pl.ds(pl.multiple_of(lax.rem(s, NP) * pw, pw), pw)
            own = pltpu.make_async_copy(o.at[:, pl.ds(pl.multiple_of(q * capd, capd), capd), cols],
                                        pan.at[b, pl.ds(core * el, el)], psem.at[b, 0])
            oth = pltpu.make_async_copy(ox.at[dp, :, :, cols], pan.at[b, pl.ds((1 - core) * el, el)], psem.at[b, 1])
            return own, oth

        def hop(i, way):
            dev = right if way == 0 else left
            src = pb.at[4 * lax.rem(i, 2), pl.ds(way * half, half), :]
            return remote(src, h1.at[way, i], h1s.at[way, i], h1r.at[way, i], dev)

        def plain(i, way):
            dev = right if way == 0 else left
            at = pl.ds((1 - way) * half, half)
            src = pb.at[4 * lax.rem(i, 2) + 1 + way, at, :]
            return remote(src, fin.at[way, i, at, :], pls.at[way, i], plr.at[way, i], dev)

        def comb(i, way):
            dev = right if way == 0 else left
            at = pl.ds(way * half, half)
            src = pb.at[4 * lax.rem(i, 2) + 1 + way, at, :]
            return remote(src, fin.at[way, i, at, :], cbs.at[way, i], cbr.at[way, i], dev)

        def hload(i):
            b = lax.rem(i, 2)
            return pltpu.make_async_copy(h.at[pl.ds(pl.multiple_of(i * tt, tt), tt), :], hb.at[b], hsem.at[b])

        def ysend(i):
            rows = pl.ds(pl.multiple_of(i * tt, tt), tt)
            return remote(yb.at[lax.rem(i, 2)], yv.at[rows, :], ys.at[i], yr.at[i], ynext)

        def wcopy(which, k, t):
            b = lax.rem(t, NW)
            if which < 3:
                src = (wq, wk, wv)[which].at[:, pl.ds(pl.multiple_of(k * WQ, WQ), WQ)]
                return pltpu.make_async_copy(src, wb.at[b, pl.ds(0, d), :], wsem.at[b])
            src = wo.at[:, pl.ds(pl.multiple_of(k * WZ, WZ), WZ)]
            return pltpu.make_async_copy(src, wb.at[b, :, pl.ds(0, WZ)], wsem.at[b])

        def wstart(t):
            r = lax.rem(t, nwp)

            @pl.when(t < nwp * len(GROUPS))
            def _():
                for which in range(3):
                    @pl.when((r >= which * nq) & (r < (which + 1) * nq))
                    def _(which=which):
                        wcopy(which, r - which * nq, t).start()

                @pl.when(r >= 3 * nq)
                def _():
                    wcopy(3, r - 3 * nq, t).start()

        def zcopy(g):
            first, count = GROUPS[g]
            return pltpu.make_async_copy(zb.at[pl.ds(0, count * tt), :], z.at[pl.ds(first * tt, count * tt), :], zsem)

        def columns(u, b):
            q = owner(lax.rem(u, 4), core)
            e = ib[b] - x * ec
            ss = sb[b]
            ok = (e >= 0) & (e < ec) & (ss >= 0)
            col = jnp.where(ok, e * capd + (ss - q * capd), -1)
            colt[...] = col.T
            gatet[...] = gb[b].T

        def gates(gm, g0, g1):
            for g in range(g0, g1):
                rows = pl.ds(16 * g, 16)
                col = colt[rows, :].astype(jnp.int16)
                gg = gatet[rows, :]
                hi = gg.astype(BF16)
                r = gg - hi.astype(F32)
                mi = r.astype(BF16)
                lw = (r - mi.astype(F32)).astype(BF16)
                cs = [jnp.broadcast_to(col[:, j:j + 1], (16, 128)) for j in range(kk)]
                ws = [[jnp.broadcast_to(p[:, j:j + 1], (16, 128)) for j in range(kk)] for p in (hi, mi, lw)]
                io = lax.broadcasted_iota(jnp.int16, (16, 128), 1)
                for v in range(kd // 128):
                    at = io + jnp.int16(128 * v)
                    t = [jnp.zeros((16, 128), BF16) for _ in range(3)]
                    for j in range(kk):
                        m = cs[j] == at
                        for k in range(3):
                            t[k] = jnp.where(m, ws[k][j], t[k])
                    for k in range(3):
                        gm[k * tt + 16 * g:k * tt + 16 * g + 16, 128 * v:128 * v + 128] = t[k]

        def finish(i):
            for way in range(2):
                plain(i, way).wait_recv()
                comb(i, way).wait_recv()
            hload(i).wait()
            b = lax.rem(i, 2)

            @pl.when(i >= 2)
            def _():
                ysend(i - 2).wait_send()

            def rows16(r, _):
                at = pl.ds(pl.multiple_of(r * 16, 16), 16)
                y = hb[b, at, :].astype(F32) + (pb[4 * b + 3, at, :] + (fin[0, i, at, :] + fin[1, i, at, :]))
                yb[b, at, :] = y.astype(BF16)
                return 0

            lax.fori_loop(0, tt // 16, rows16, 0)
            ysend(i).start()

        def attend(g):
            first, count = GROUPS[g]
            base, m = first * tt, count * tt
            nk = base + m
            t0 = nwp * g
            for j in range(first, first + count):
                ysend(j).wait_recv()

            def norm(r, _):
                for a in range(4):
                    at = pl.ds(pl.multiple_of(r * 64 + a * 16, 16), 16)
                    y = yv[pl.ds(pl.multiple_of(base + r * 64 + a * 16, 16), 16), :].astype(F32)
                    xf = y * lax.rsqrt(jnp.mean(y * y, axis=-1, keepdims=True) + EPS) * nw[...]
                    xb[at, :] = xf.astype(BF16)
                return 0

            lax.fori_loop(0, m // 64, norm, 0)

            def project(k, _):
                t = t0 + k
                wcopy(0, 0, t).wait()
                r = jnp.dot(xb[0:m], wb[lax.rem(t, NW), 0:d, :], preferred_element_type=F32).astype(BF16)
                cols = pl.ds(pl.multiple_of(lax.rem(k, nq) * WQ, WQ), WQ)

                @pl.when(k < nq)
                def _():
                    qb[0:m, cols] = r

                @pl.when(k >= nq)
                def _():
                    kv[k // nq - 1, base:base + m, cols] = r

                wstart(t + NW)
                return 0

            lax.fori_loop(0, 3 * nq, project, 0)

            def heads(v, _):
                cl = [pl.ds(pl.multiple_of((NB * v + a) * HEAD, HEAD), HEAD) for a in range(NB)]
                ss = [lax.dot_general(qb[0:m, cs], kv[0, 0:nk, cs], (((1,), (1,)), ((), ())), preferred_element_type=F32) for cs in cl]
                keep = lax.broadcasted_iota(jnp.int32, (m, m), 0) >= lax.broadcasted_iota(jnp.int32, (m, m), 1)
                sm = []
                for sc in ss:
                    last = jnp.where(keep, sc[:, base:], -1e30)
                    sm.append(jnp.concatenate([sc[:, :base], last], axis=1) if base else last)
                mx = [jnp.max(sc, axis=-1, keepdims=True) for sc in sm]
                ps = [jnp.exp2((sc - mm) * SCALE2) for sc, mm in zip(sm, mx)]
                rs = [1.0 / jnp.sum(p, axis=-1, keepdims=True) for p in ps]
                pr = [(p * r).astype(BF16) for p, r in zip(ps, rs)]
                at = [jnp.dot(p, kv[1, 0:nk, cs], preferred_element_type=F32).astype(BF16) for p, cs in zip(pr, cl)]
                for v_, cs in zip(at, cl):
                    ab[0:m, cs] = v_
                return 0

            lax.fori_loop(0, nh // NB, heads, 0)
            if g >= 1:
                zcopy(g - 1).wait()

            def out(k, _):
                t = t0 + 3 * nq + k
                wcopy(3, 0, t).wait()
                r = jnp.dot(ab[0:m], wb[lax.rem(t, NW), :, 0:WZ], preferred_element_type=F32).astype(BF16)
                cols = pl.ds(pl.multiple_of(k * WZ, WZ), WZ)
                zb[0:m, cols] = (yv[base:base + m, cols].astype(F32) + r.astype(F32)).astype(BF16)
                wstart(t + NW)
                return 0

            lax.fori_loop(0, nz, out, 0)
            zcopy(g).start()

        def unit(u, gmc, gmn, bn):
            dst = lax.rem(u, 8)

            @pl.when(u + 1 < nu)
            def _():
                for cp in small(u + 1):
                    cp.wait()

            columns(u + 1, bn)

            @pl.when(u + 3 < nu)
            def _():
                for cp in small(u + 3):
                    cp.start()

            ng = tt // 16 // NP
            for k in range(NP):
                s = NP * u + k
                nxt = s + NS - 1

                @pl.when((nxt < 4 * NP) & (lax.rem(nxt, NP) == 0))
                def _(nxt=nxt):
                    exch(nxt // NP).wait_recv()

                @pl.when(nxt < nu * NP)
                def _(nxt=nxt):
                    for cp in panel(nxt):
                        cp.start()

                for cp in panel(s):
                    cp.wait()
                w = pan[lax.rem(s, NS)].reshape(kd, pw)
                acc = jnp.dot(gmc[...], w, preferred_element_type=F32)
                pb[dst, :, k * pw:(k + 1) * pw] = acc[0:tt] + (acc[tt:2 * tt] + acc[2 * tt:3 * tt])
                gates(gmn, ng * k, ng * (k + 1))

        bar = pltpu.get_barrier_semaphore()
        for dev in (partner, right, left, ynext, yprev):
            pl.semaphore_signal(bar, inc=1, device_id=dev, device_id_type=MESH)
        pl.semaphore_wait(bar, 5)

        for dp in range(4):
            exch(dp).start()
        for u in range(2):
            for cp in small(u):
                cp.start()
        for t in range(NW):
            wstart(jnp.int32(t))
        for cp in small(0):
            cp.wait()
        columns(jnp.int32(0), 0)
        for cp in small(2):
            cp.start()
        hload(0).start()
        gates(gm0, 0, tt // 16)
        exch(0).wait_recv()
        for s in range(NS - 1):
            for cp in panel(s):
                cp.start()

        unit(jnp.int32(0), gm0, gm1, 1)
        hop(jnp.int32(0), 0).start()
        hop(jnp.int32(0), 1).start()

        def iteration(i, _):
            @pl.when(i < npair)
            def _():
                def two(v, _):
                    u = 4 * i + 2 * v + 1
                    unit(u, gm1, gm0, 0)

                    @pl.when(v == 0)
                    def _():
                        plain(i, 0).start()

                    @pl.when(v == 1)
                    def _():
                        for way in range(2):
                            hop(i, way).wait_recv()
                            src = 4 * lax.rem(i, 2) + 1 + way

                            def add(r, _, way=way, src=src):
                                at = pl.ds(pl.multiple_of(way * half + r * 16, 16), 16)
                                pb[src, at, :] = pb[src, at, :] + h1[way, i, pl.ds(pl.multiple_of(r * 16, 16), 16), :]
                                return 0

                            lax.fori_loop(0, half // 16, add, 0)
                            comb(i, way).start()

                        @pl.when(i >= 1)
                        def _():
                            for way in range(2):
                                hop(i - 1, way).wait_send()
                                plain(i - 1, way).wait_send()
                                comb(i - 1, way).wait_send()

                    @pl.when(u + 1 < nu)
                    def _():
                        unit(u + 1, gm0, gm1, 1)

                        @pl.when(v == 0)
                        def _():
                            plain(i, 1).start()

                        @pl.when(v == 1)
                        def _():
                            hop(i + 1, 0).start()
                            hop(i + 1, 1).start()
                    return 0

                lax.fori_loop(0, 2, two, 0)

            @pl.when((i >= 1) & (i <= npair))
            def _():
                finish(i - 1)

            @pl.when(i + 1 < npair)
            def _():
                hload(i + 1).start()

            for g, (first, count) in enumerate(GROUPS):
                @pl.when(i == first + count + 1)
                def _(g=g):
                    attend(g)
            return 0

        lax.fori_loop(0, npair + 2, iteration, 0)
        for dp in range(4):
            exch(dp).wait_send()
        for way in range(2):
            hop(npair - 1, way).wait_send()
            plain(npair - 1, way).wait_send()
            comb(npair - 1, way).wait_send()
        for i in range(npair - 2, npair):
            ysend(i).wait_send()
        zcopy(len(GROUPS) - 1).wait()

    dma = pltpu.SemaphoreType.DMA
    anyspec = pl.BlockSpec(memory_space=pl.ANY)
    flops = 2 * 3 * 4 * ln * kd * d
    return pl.pallas_call(
        kernel,
        out_shape=(jax.ShapeDtypeStruct((ln, d), BF16), jax.ShapeDtypeStruct((4, el, capd, d), BF16)),
        in_specs=[anyspec] * 5 + [pl.BlockSpec(memory_space=pltpu.VMEM)] + [anyspec] * 4,
        out_specs=(anyspec, anyspec),
        scratch_shapes=[
            pltpu.VMEM((NS, ec, capd, pw), BF16),
            pltpu.VMEM((3 * tt, kd), BF16),
            pltpu.VMEM((3 * tt, kd), BF16),
            pltpu.VMEM((tt, kk), jnp.int32),
            pltpu.VMEM((tt, kk), F32),
            pltpu.VMEM((8, tt, d), F32),
            pltpu.VMEM((2, npair, half, d), F32),
            pltpu.VMEM((2, npair, tt, d), F32),
            pltpu.VMEM((2, kk, tt), jnp.int32),
            pltpu.VMEM((2, kk, tt), jnp.int32),
            pltpu.VMEM((2, kk, tt), F32),
            pltpu.VMEM((2, tt, d), BF16),
            pltpu.VMEM((2, tt, d), BF16),
            pltpu.VMEM((ln, d), BF16),
            pltpu.VMEM((mg, d), BF16),
            pltpu.VMEM((NW, hd, WQ), BF16),
            pltpu.VMEM((mg, hd), BF16),
            pltpu.VMEM((2, ln, hd), BF16),
            pltpu.VMEM((mg, hd), BF16),
            pltpu.VMEM((mg, d), BF16),
            dma((4,)), dma((4,)),
            dma((2, npair)), dma((2, npair)), dma((2, npair)), dma((2, npair)), dma((2, npair)), dma((2, npair)),
            dma((npair,)), dma((npair,)),
            dma((NS, 2)), dma((2, 3)), dma((2,)), dma((NW,)), dma,
        ],
        compiler_params=pltpu.CompilerParams(collective_id=1, has_side_effects=True, vmem_limit_bytes=67043328),
        cost_estimate=pl.CostEstimate(flops=flops, bytes_accessed=200 << 20, transcendentals=0),
        name='stage',
    )


def solution(mesh):
    n = mesh.shape['ep']
    npp = mesh.shape['pp']
    sp_o = P('pp', 'data', 'ep', None, None)
    sp_r = P('pp', 'data', None, None, None)
    sp_1 = P('pp', None)
    sp_w = P('pp', None, None)

    def body(o, idx, slot, gate, h, norm_w, wq, wk, wv, wo):
        _, nm, el, c, d = o.shape
        ln, kk = h.shape[3], idx.shape[4]
        hd = wq.shape[2]
        assert nm == 1 and h.shape[2] == 1
        stage = make_stage(n, npp, el, c, d, ln, kk, hd)
        turn = [jnp.swapaxes(a.reshape(n, ln, kk), 1, 2) for a in (idx, slot, gate)]
        z, _ = stage(o.reshape(el, c, d), *turn, h.reshape(ln, d), norm_w, wq[0], wk[0], wv[0], wo[0])
        return z.reshape(h.shape)

    return jax.shard_map(body, mesh=mesh, in_specs=(sp_o, sp_r, sp_r, sp_r, sp_o, sp_1, sp_w, sp_w, sp_w, sp_w), out_specs=sp_o, check_vma=False)
```

```python
import jax
import jax.numpy as jnp
from jax import lax
from jax.experimental import pallas as pl
from jax.experimental.pallas import tpu as pltpu
from jax.sharding import PartitionSpec as P

HEAD = 128
EPS = 1e-6
SCALE2 = HEAD ** -0.5 * 1.4426950408889634
MESH = pl.DeviceIdType.MESH
F32 = jnp.float32
BF16 = jnp.bfloat16
HALF = 64
NS = 3
NP = 2
NW = 3
NB = 4
GROUPS = ((0, 2), (2, 2), (4, 1), (5, 1))
WQ = 512
WZ = 256


def make_stage(n, npp, el, c, d, ln, kk, hd):
    nx = n // 2
    assert nx == 4
    capd = c // n
    ec = 2 * el
    kd = ec * capd
    tt = 2 * HALF
    npair = ln // tt
    nu = 4 * npair
    pw = d // NP
    half = HALF
    qt = half // 2
    nq = hd // WQ
    nz = d // WZ
    nwp = 3 * nq + nz
    nh = hd // HEAD
    mg = tt * max(count for _, count in GROUPS)
    assert sum(count for _, count in GROUPS) == npair

    def kernel(o, idx, slot, gate, h, nw, wq, wk, wv, wo, z, ox,
               pan, gm0, gm1, colt, gatet, pb, h1, fin, ib, sb, gb, hb, yb, yv, xb, wb, qb, kv, ab, zb,
               xs, xr, h1s, h1r, pls, plr, cbs, cbr, ys, yr, psem, isem, hsem, wsem, zsem):
        ep = lax.axis_index('ep')
        pp = lax.axis_index('pp')
        core = lax.rem(ep, 2)
        x = ep // 2
        partner = {'ep': 2 * x + 1 - core}
        right = {'ep': 2 * lax.rem(x + 1, nx) + core}
        left = {'ep': 2 * lax.rem(x + nx - 1, nx) + core}
        ynext = {'pp': lax.rem(pp + 1, npp)}
        yprev = {'pp': lax.rem(pp + npp - 1, npp)}

        def remote(src, dst, ss, rs, dev):
            return pltpu.make_async_remote_copy(src_ref=src, dst_ref=dst, send_sem=ss, recv_sem=rs, device_id=dev, device_id_type=MESH)

        def owner(dp, cc):
            dd = jnp.where(dp == 0, 2, jnp.where(dp == 1, 1, jnp.where(dp == 2, 3, 0)))
            return 2 * lax.rem(x + dd, nx) + cc

        def exch(s):
            dp = s // NP
            q = owner(dp, 1 - core)
            cols = pl.ds(pl.multiple_of(lax.rem(s, NP) * pw, pw), pw)
            src = o.at[:, pl.ds(pl.multiple_of(q * capd, capd), capd), cols]
            return remote(src, ox.at[dp, :, :, cols], xs.at[s], xr.at[s], partner)

        def small(u):
            i = u // 4
            q = owner(lax.rem(u, 4), core)
            b = lax.rem(u, 2)
            cols = pl.ds(pl.multiple_of(i * tt, tt), tt)
            return [pltpu.make_async_copy(a.at[q, :, cols], v.at[b], isem.at[b, k])
                    for k, (a, v) in enumerate(((idx, ib), (slot, sb), (gate, gb)))]

        def panel(s):
            u = s // NP
            dp = lax.rem(u, 4)
            q = owner(dp, core)
            b = lax.rem(s, NS)
            cols = pl.ds(pl.multiple_of(lax.rem(s, NP) * pw, pw), pw)
            own = pltpu.make_async_copy(o.at[:, pl.ds(pl.multiple_of(q * capd, capd), capd), cols],
                                        pan.at[b, pl.ds(core * el, el)], psem.at[b, 0])
            oth = pltpu.make_async_copy(ox.at[dp, :, :, cols], pan.at[b, pl.ds((1 - core) * el, el)], psem.at[b, 1])
            return own, oth

        def hop(i, way):
            dev = right if way == 0 else left
            src = pb.at[4 * lax.rem(i, 2), pl.ds(way * half, half), :]
            return remote(src, h1.at[way, i], h1s.at[way, i], h1r.at[way, i], dev)

        def plain(i, way):
            dev = right if way == 0 else left
            at = pl.ds((1 - way) * half, half)
            src = pb.at[4 * lax.rem(i, 2) + 1 + way, at, :]
            return remote(src, fin.at[way, i, at, :], pls.at[way, i], plr.at[way, i], dev)

        def comb(i, way, a):
            dev = right if way == 0 else left
            at = pl.ds(way * half + a * qt, qt)
            src = pb.at[4 * lax.rem(i, 2) + 1 + way, at, :]
            return remote(src, fin.at[way, i, at, :], cbs.at[way, i, a], cbr.at[way, i, a], dev)

        def hload(i):
            b = lax.rem(i, 2)
            return pltpu.make_async_copy(h.at[pl.ds(pl.multiple_of(i * tt, tt), tt), :], hb.at[b], hsem.at[b])

        def ysend(i, a, way):
            at = way * half + a * qt
            rows = pl.ds(pl.multiple_of(i * tt + at, qt), qt)
            return remote(yb.at[lax.rem(i, 2), pl.ds(at, qt), :], yv.at[rows, :], ys.at[i, a, way], yr.at[i, a, way], ynext)

        def wcopy(which, k, t):
            b = lax.rem(t, NW)
            if which < 3:
                src = (wq, wk, wv)[which].at[:, pl.ds(pl.multiple_of(k * WQ, WQ), WQ)]
                return pltpu.make_async_copy(src, wb.at[b, pl.ds(0, d), :], wsem.at[b])
            src = wo.at[:, pl.ds(pl.multiple_of(k * WZ, WZ), WZ)]
            return pltpu.make_async_copy(src, wb.at[b, :, pl.ds(0, WZ)], wsem.at[b])

        def wstart(t):
            r = lax.rem(t, nwp)

            @pl.when(t < nwp * len(GROUPS))
            def _():
                for which in range(3):
                    @pl.when((r >= which * nq) & (r < (which + 1) * nq))
                    def _(which=which):
                        wcopy(which, r - which * nq, t).start()

                @pl.when(r >= 3 * nq)
                def _():
                    wcopy(3, r - 3 * nq, t).start()

        def zcopy(g):
            first, count = GROUPS[g]
            return pltpu.make_async_copy(zb.at[pl.ds(0, count * tt), :], z.at[pl.ds(first * tt, count * tt), :], zsem)

        def columns(u, b):
            q = owner(lax.rem(u, 4), core)
            e = ib[b] - x * ec
            ss = sb[b]
            ok = (e >= 0) & (e < ec) & (ss >= 0)
            col = jnp.where(ok, e * capd + (ss - q * capd), -1)
            colt[...] = col.T
            gatet[...] = gb[b].T

        def gates(gm, g0, g1):
            for g in range(g0, g1):
                rows = pl.ds(16 * g, 16)
                col = colt[rows, :].astype(jnp.int16)
                gg = gatet[rows, :]
                hi = gg.astype(BF16)
                r = gg - hi.astype(F32)
                mi = r.astype(BF16)
                lw = (r - mi.astype(F32)).astype(BF16)
                cs = [jnp.broadcast_to(col[:, j:j + 1], (16, 128)) for j in range(kk)]
                ws = [[jnp.broadcast_to(p[:, j:j + 1], (16, 128)) for j in range(kk)] for p in (hi, mi, lw)]
                io = lax.broadcasted_iota(jnp.int16, (16, 128), 1)
                for v in range(kd // 128):
                    at = io + jnp.int16(128 * v)
                    t = [jnp.zeros((16, 128), BF16) for _ in range(3)]
                    for j in range(kk):
                        m = cs[j] == at
                        for k in range(3):
                            t[k] = jnp.where(m, ws[k][j], t[k])
                    for k in range(3):
                        gm[k * tt + 16 * g:k * tt + 16 * g + 16, 128 * v:128 * v + 128] = t[k]

        def finish(i):
            b = lax.rem(i, 2)

            @pl.when(i >= 2)
            def _():
                for a, way in parts:
                    ysend(i - 2, a, way).wait_send()

            hload(i).wait()
            for way in range(2):
                plain(i, way).wait_recv()
            for a in range(2):
                for way in range(2):
                    comb(i, way, a).wait_recv()

                def rows16(r, _, a=a):
                    for way in range(2):
                        at = pl.ds(pl.multiple_of(way * half + a * qt + r * 16, 16), 16)
                        y = hb[b, at, :].astype(F32) + (pb[4 * b + 3, at, :] + (fin[0, i, at, :] + fin[1, i, at, :]))
                        yb[b, at, :] = y.astype(BF16)
                    return 0

                lax.fori_loop(0, qt // 16, rows16, 0)
                for way in range(2):
                    ysend(i, a, way).start()

        def attend(g, head=True, tail=True):
            first, count = GROUPS[g]
            base, m = first * tt, count * tt
            nk = base + m
            t0 = nwp * g

            def norm(r, _):
                for a in range(4):
                    at = pl.ds(pl.multiple_of(r * 64 + a * 16, 16), 16)
                    y = yv[pl.ds(pl.multiple_of(base + r * 64 + a * 16, 16), 16), :].astype(F32)
                    xf = y * lax.rsqrt(jnp.mean(y * y, axis=-1, keepdims=True) + EPS) * nw[...]
                    xb[at, :] = xf.astype(BF16)
                return 0

            if head:
                for j in range(first, first + count):
                    for a, way in parts:
                        ysend(j, a, way).wait_recv()
                lax.fori_loop(0, m // 64, norm, 0)

            def project(k, _):
                t = t0 + k
                wcopy(0, 0, t).wait()
                r = jnp.dot(xb[0:m], wb[lax.rem(t, NW), 0:d, :], preferred_element_type=F32).astype(BF16)
                cols = pl.ds(pl.multiple_of(lax.rem(k, nq) * WQ, WQ), WQ)

                @pl.when(k < nq)
                def _():
                    qb[0:m, cols] = r

                @pl.when(k >= nq)
                def _():
                    kv[k // nq - 1, base:base + m, cols] = r

                wstart(t + NW)
                return 0

            if head:
                lax.fori_loop(0, 3 * nq, project, 0)
            if not tail:
                return

            def heads(v, _):
                cl = [pl.ds(pl.multiple_of((NB * v + a) * HEAD, HEAD), HEAD) for a in range(NB)]
                ss = [lax.dot_general(qb[0:m, cs], kv[0, 0:nk, cs], (((1,), (1,)), ((), ())), preferred_element_type=F32) for cs in cl]
                keep = lax.broadcasted_iota(jnp.int32, (m, m), 0) >= lax.broadcasted_iota(jnp.int32, (m, m), 1)
                sm = []
                for sc in ss:
                    last = jnp.where(keep, sc[:, base:], -1e30)
                    sm.append(jnp.concatenate([sc[:, :base], last], axis=1) if base else last)
                mx = [jnp.max(sc, axis=-1, keepdims=True) for sc in sm]
                ps = [jnp.exp2((sc - mm) * SCALE2) for sc, mm in zip(sm, mx)]
                rs = [1.0 / jnp.sum(p, axis=-1, keepdims=True) for p in ps]
                pr = [(p * r).astype(BF16) for p, r in zip(ps, rs)]
                at = [jnp.dot(p, kv[1, 0:nk, cs], preferred_element_type=F32).astype(BF16) for p, cs in zip(pr, cl)]
                for v_, cs in zip(at, cl):
                    ab[0:m, cs] = v_
                return 0

            lax.fori_loop(0, nh // NB, heads, 0)
            if g >= 1:
                zcopy(g - 1).wait()

            def out(k, _):
                t = t0 + 3 * nq + k
                wcopy(3, 0, t).wait()
                r = jnp.dot(ab[0:m], wb[lax.rem(t, NW), :, 0:WZ], preferred_element_type=F32).astype(BF16)
                cols = pl.ds(pl.multiple_of(k * WZ, WZ), WZ)
                zb[0:m, cols] = (yv[base:base + m, cols].astype(F32) + r.astype(F32)).astype(BF16)
                wstart(t + NW)
                return 0

            lax.fori_loop(0, nz, out, 0)
            zcopy(g).start()

        parts = [(a, way) for a in range(2) for way in range(2)]

        def unit(u, gmc, gmn, bn, first=False):
            dst = lax.rem(u, 8)

            @pl.when(u + 1 < nu)
            def _():
                for cp in small(u + 1):
                    cp.wait()

            columns(u + 1, bn)

            @pl.when(u + 3 < nu)
            def _():
                for cp in small(u + 3):
                    cp.start()

            ng = tt // 16 // NP
            for k in range(NP):
                s = NP * u + k
                nxt = s + NS - 1

                @pl.when((nxt >= 4 * NP) & (nxt < nu * NP))
                def _(nxt=nxt):
                    for cp in panel(nxt):
                        cp.start()

                for cp in panel(s):
                    cp.wait()
                w = pan[lax.rem(s, NS)].reshape(kd, pw)
                acc = jnp.dot(gmc[...], w, preferred_element_type=F32)
                pb[dst, :, k * pw:(k + 1) * pw] = acc[0:tt] + (acc[tt:2 * tt] + acc[2 * tt:3 * tt])
                gates(gmn, ng * k, ng * (k + 1))
                early = s + 1 if first else nxt

                if not first or k < NP - 1:
                    @pl.when(early < 4 * NP)
                    def _(early=early):
                        exch(early).wait_recv()
                        for cp in panel(early):
                            cp.start()

        bar = pltpu.get_barrier_semaphore()
        for dev in (partner, right, left, ynext, yprev):
            pl.semaphore_signal(bar, inc=1, device_id=dev, device_id_type=MESH)
        pl.semaphore_wait(bar, 5)

        for s in range(4 * NP):
            exch(jnp.int32(s)).start()
        for u in range(2):
            for cp in small(u):
                cp.start()
        for t in range(NW):
            wstart(jnp.int32(t))
        for cp in small(0):
            cp.wait()
        columns(jnp.int32(0), 0)
        for cp in small(2):
            cp.start()
        hload(0).start()
        gates(gm0, 0, tt // 16)
        exch(jnp.int32(0)).wait_recv()
        for cp in panel(jnp.int32(0)):
            cp.start()

        unit(jnp.int32(0), gm0, gm1, 1, True)
        hop(jnp.int32(0), 0).start()
        hop(jnp.int32(0), 1).start()
        for s in range(NP, NS + 1):
            exch(jnp.int32(s)).wait_recv()
            for cp in panel(jnp.int32(s)):
                cp.start()

        def iteration(i, _):
            def two(v, _):
                u = 4 * i + 2 * v + 1
                unit(u, gm1, gm0, 0)

                @pl.when(v == 0)
                def _():
                    plain(i, 0).start()

                @pl.when(v == 1)
                def _():
                    @pl.when(i >= 1)
                    def _():
                        finish(i - 1)

                    @pl.when(i + 1 < npair)
                    def _():
                        hload(i + 1).start()

                    for g, (first, count) in enumerate(GROUPS):
                        if first + count + 1 < npair:
                            @pl.when(i == first + count + 1)
                            def _(g=g):
                                attend(g)

                    for way in range(2):
                        hop(i, way).wait_recv()
                        src = 4 * lax.rem(i, 2) + 1 + way

                        def add(r, _, way=way, src=src):
                            at = pl.ds(pl.multiple_of(way * half + r * 16, 16), 16)
                            pb[src, at, :] = pb[src, at, :] + h1[way, i, pl.ds(pl.multiple_of(r * 16, 16), 16), :]
                            return 0

                        lax.fori_loop(0, half // 16, add, 0)
                        for a in range(2):
                            comb(i, way, a).start()

                    @pl.when(i >= 1)
                    def _():
                        for way in range(2):
                            hop(i - 1, way).wait_send()
                            plain(i - 1, way).wait_send()
                            for a in range(2):
                                comb(i - 1, way, a).wait_send()

                @pl.when(u + 1 < nu)
                def _():
                    unit(u + 1, gm0, gm1, 1)

                    @pl.when(v == 0)
                    def _():
                        plain(i, 1).start()

                    @pl.when(v == 1)
                    def _():
                        hop(i + 1, 0).start()
                        hop(i + 1, 1).start()
                return 0

            lax.fori_loop(0, 2, two, 0)
            return 0

        lax.fori_loop(0, npair, iteration, 0)
        attend(2, tail=False)
        finish(jnp.int32(npair - 1))
        attend(2, head=False)
        attend(3)
        for s in range(4 * NP):
            exch(jnp.int32(s)).wait_send()
        for way in range(2):
            hop(npair - 1, way).wait_send()
            plain(npair - 1, way).wait_send()
            for a in range(2):
                comb(npair - 1, way, a).wait_send()
        for i in range(npair - 2, npair):
            for a, way in parts:
                ysend(i, a, way).wait_send()
        zcopy(len(GROUPS) - 1).wait()

    dma = pltpu.SemaphoreType.DMA
    anyspec = pl.BlockSpec(memory_space=pl.ANY)
    flops = 2 * 3 * 4 * ln * kd * d
    return pl.pallas_call(
        kernel,
        out_shape=(jax.ShapeDtypeStruct((ln, d), BF16), jax.ShapeDtypeStruct((4, el, capd, d), BF16)),
        in_specs=[anyspec] * 5 + [pl.BlockSpec(memory_space=pltpu.VMEM)] + [anyspec] * 4,
        out_specs=(anyspec, anyspec),
        scratch_shapes=[
            pltpu.VMEM((NS, ec, capd, pw), BF16),
            pltpu.VMEM((3 * tt, kd), BF16),
            pltpu.VMEM((3 * tt, kd), BF16),
            pltpu.VMEM((tt, kk), jnp.int32),
            pltpu.VMEM((tt, kk), F32),
            pltpu.VMEM((8, tt, d), F32),
            pltpu.VMEM((2, npair, half, d), F32),
            pltpu.VMEM((2, npair, tt, d), F32),
            pltpu.VMEM((2, kk, tt), jnp.int32),
            pltpu.VMEM((2, kk, tt), jnp.int32),
            pltpu.VMEM((2, kk, tt), F32),
            pltpu.VMEM((2, tt, d), BF16),
            pltpu.VMEM((2, tt, d), BF16),
            pltpu.VMEM((ln, d), BF16),
            pltpu.VMEM((mg, d), BF16),
            pltpu.VMEM((NW, hd, WQ), BF16),
            pltpu.VMEM((mg, hd), BF16),
            pltpu.VMEM((2, ln, hd), BF16),
            pltpu.VMEM((mg, hd), BF16),
            pltpu.VMEM((mg, d), BF16),
            dma((4 * NP,)), dma((4 * NP,)),
            dma((2, npair)), dma((2, npair)), dma((2, npair)), dma((2, npair)), dma((2, npair, 2)), dma((2, npair, 2)),
            dma((npair, 2, 2)), dma((npair, 2, 2)),
            dma((NS, 2)), dma((2, 3)), dma((2,)), dma((NW,)), dma,
        ],
        compiler_params=pltpu.CompilerParams(collective_id=1, has_side_effects=True, vmem_limit_bytes=67043328),
        cost_estimate=pl.CostEstimate(flops=flops, bytes_accessed=200 << 20, transcendentals=0),
        name='stage',
    )


def solution(mesh):
    n = mesh.shape['ep']
    npp = mesh.shape['pp']
    sp_o = P('pp', 'data', 'ep', None, None)
    sp_r = P('pp', 'data', None, None, None)
    sp_1 = P('pp', None)
    sp_w = P('pp', None, None)

    def body(o, idx, slot, gate, h, norm_w, wq, wk, wv, wo):
        _, nm, el, c, d = o.shape
        ln, kk = h.shape[3], idx.shape[4]
        hd = wq.shape[2]
        assert nm == 1 and h.shape[2] == 1
        stage = make_stage(n, npp, el, c, d, ln, kk, hd)
        turn = [jnp.swapaxes(a.reshape(n, ln, kk), 1, 2) for a in (idx, slot, gate)]
        z, _ = stage(o.reshape(el, c, d), *turn, h.reshape(ln, d), norm_w, wq[0], wk[0], wv[0], wo[0])
        return z.reshape(h.shape)

    return jax.shard_map(body, mesh=mesh, in_specs=(sp_o, sp_r, sp_r, sp_r, sp_o, sp_1, sp_w, sp_w, sp_w, sp_w), out_specs=sp_o, check_vma=False)
```

```python
import jax
import jax.numpy as jnp
from jax import lax
from jax.experimental import pallas as pl
from jax.experimental.pallas import tpu as pltpu
from jax.sharding import PartitionSpec as P

HEAD = 128
EPS = 1e-6
SCALE2 = HEAD ** -0.5 * 1.4426950408889634
MESH = pl.DeviceIdType.MESH
F32 = jnp.float32
BF16 = jnp.bfloat16
HALF = 64
NS = 3
NP = 2
NW = 3
NB = 4
GROUPS = ((0, 2), (2, 2), (4, 1), (5, 1))
WQ = 512
WZ = 256


def make_stage(n, npp, el, c, d, ln, kk, hd):
    nx = n // 2
    assert nx == 4
    capd = c // n
    ec = 2 * el
    kd = ec * capd
    tt = 2 * HALF
    npair = ln // tt
    nu = 4 * npair
    pw = d // NP
    half = HALF
    qt = half // 2
    nq = hd // WQ
    nz = d // WZ
    nwp = 3 * nq + nz
    assert WQ == NB * HEAD
    mg = tt * max(count for _, count in GROUPS)
    assert sum(count for _, count in GROUPS) == npair

    def kernel(o, idx, slot, gate, h, nw, wq, wk, wv, wo, z, ox,
               pan, gm0, gm1, colt, gatet, pb, h1, fin, ib, sb, gb, hb, yb, yv, xb, wb, qb, kv, ab, zb,
               xs, xr, h1s, h1r, pls, plr, cbs, cbr, ys, yr, psem, isem, hsem, wsem, zsem):
        ep = lax.axis_index('ep')
        pp = lax.axis_index('pp')
        core = lax.rem(ep, 2)
        x = ep // 2
        partner = {'ep': 2 * x + 1 - core}
        right = {'ep': 2 * lax.rem(x + 1, nx) + core}
        left = {'ep': 2 * lax.rem(x + nx - 1, nx) + core}
        ynext = {'pp': lax.rem(pp + 1, npp)}
        yprev = {'pp': lax.rem(pp + npp - 1, npp)}

        def remote(src, dst, ss, rs, dev):
            return pltpu.make_async_remote_copy(src_ref=src, dst_ref=dst, send_sem=ss, recv_sem=rs, device_id=dev, device_id_type=MESH)

        def owner(dp, cc):
            dd = jnp.where(dp == 0, 2, jnp.where(dp == 1, 1, jnp.where(dp == 2, 3, 0)))
            return 2 * lax.rem(x + dd, nx) + cc

        def exch(s):
            dp = s // NP
            q = owner(dp, 1 - core)
            cols = pl.ds(pl.multiple_of(lax.rem(s, NP) * pw, pw), pw)
            src = o.at[:, pl.ds(pl.multiple_of(q * capd, capd), capd), cols]
            return remote(src, ox.at[dp, :, :, cols], xs.at[s], xr.at[s], partner)

        def small(u):
            i = u // 4
            q = owner(lax.rem(u, 4), core)
            b = lax.rem(u, 2)
            cols = pl.ds(pl.multiple_of(i * tt, tt), tt)
            return [pltpu.make_async_copy(a.at[q, :, cols], v.at[b], isem.at[b, k])
                    for k, (a, v) in enumerate(((idx, ib), (slot, sb), (gate, gb)))]

        def panel(s):
            u = s // NP
            dp = lax.rem(u, 4)
            q = owner(dp, core)
            b = lax.rem(s, NS)
            cols = pl.ds(pl.multiple_of(lax.rem(s, NP) * pw, pw), pw)
            own = pltpu.make_async_copy(o.at[:, pl.ds(pl.multiple_of(q * capd, capd), capd), cols],
                                        pan.at[b, pl.ds(core * el, el)], psem.at[b, 0])
            oth = pltpu.make_async_copy(ox.at[dp, :, :, cols], pan.at[b, pl.ds((1 - core) * el, el)], psem.at[b, 1])
            return own, oth

        def hop(i, way):
            dev = right if way == 0 else left
            src = pb.at[4 * lax.rem(i, 2), pl.ds(way * half, half), :]
            return remote(src, h1.at[way, i], h1s.at[way, i], h1r.at[way, i], dev)

        def plain(i, way):
            dev = right if way == 0 else left
            at = pl.ds((1 - way) * half, half)
            src = pb.at[4 * lax.rem(i, 2) + 1 + way, at, :]
            return remote(src, fin.at[way, i, at, :], pls.at[way, i], plr.at[way, i], dev)

        def comb(i, way, a):
            dev = right if way == 0 else left
            at = pl.ds(way * half + a * qt, qt)
            src = pb.at[4 * lax.rem(i, 2) + 1 + way, at, :]
            return remote(src, fin.at[way, i, at, :], cbs.at[way, i, a], cbr.at[way, i, a], dev)

        def hload(i):
            b = lax.rem(i, 2)
            return pltpu.make_async_copy(h.at[pl.ds(pl.multiple_of(i * tt, tt), tt), :], hb.at[b], hsem.at[b])

        def ysend(i, a, way):
            at = way * half + a * qt
            rows = pl.ds(pl.multiple_of(i * tt + at, qt), qt)
            return remote(yb.at[lax.rem(i, 2), pl.ds(at, qt), :], yv.at[rows, :], ys.at[i, a, way], yr.at[i, a, way], ynext)

        def wcopy(which, k, t):
            b = lax.rem(t, NW)
            if which < 3:
                src = (wq, wk, wv)[which].at[:, pl.ds(pl.multiple_of(k * WQ, WQ), WQ)]
                return pltpu.make_async_copy(src, wb.at[b, pl.ds(0, d), :], wsem.at[b])
            src = wo.at[:, pl.ds(pl.multiple_of(k * WZ, WZ), WZ)]
            return pltpu.make_async_copy(src, wb.at[b, :, pl.ds(0, WZ)], wsem.at[b])

        def wstart(t):
            r = lax.rem(t, nwp)

            @pl.when(t < nwp * len(GROUPS))
            def _():
                for which in range(3):
                    @pl.when((r < 3 * nq) & (lax.rem(r, 3) == which))
                    def _(which=which):
                        wcopy(which, r // 3, t).start()

                @pl.when(r >= 3 * nq)
                def _():
                    wcopy(3, r - 3 * nq, t).start()

        def zcopy(g):
            first, count = GROUPS[g]
            return pltpu.make_async_copy(zb.at[pl.ds(0, count * tt), :], z.at[pl.ds(first * tt, count * tt), :], zsem)

        def columns(u, b):
            q = owner(lax.rem(u, 4), core)
            e = ib[b] - x * ec
            ss = sb[b]
            ok = (e >= 0) & (e < ec) & (ss >= 0)
            col = jnp.where(ok, e * capd + (ss - q * capd), -1)
            colt[...] = col.T
            gatet[...] = gb[b].T

        def gates(gm, g0, g1):
            for g in range(g0, g1):
                rows = pl.ds(16 * g, 16)
                col = colt[rows, :].astype(jnp.int16)
                gg = gatet[rows, :]
                hi = gg.astype(BF16)
                r = gg - hi.astype(F32)
                mi = r.astype(BF16)
                lw = (r - mi.astype(F32)).astype(BF16)
                cs = [jnp.broadcast_to(col[:, j:j + 1], (16, 128)) for j in range(kk)]
                ws = [[jnp.broadcast_to(p[:, j:j + 1], (16, 128)) for j in range(kk)] for p in (hi, mi, lw)]
                io = lax.broadcasted_iota(jnp.int16, (16, 128), 1)
                for v in range(kd // 128):
                    at = io + jnp.int16(128 * v)
                    t = [jnp.zeros((16, 128), BF16) for _ in range(3)]
                    for j in range(kk):
                        m = cs[j] == at
                        for k in range(3):
                            t[k] = jnp.where(m, ws[k][j], t[k])
                    for k in range(3):
                        gm[k * tt + 16 * g:k * tt + 16 * g + 16, 128 * v:128 * v + 128] = t[k]

        def finish(i):
            b = lax.rem(i, 2)

            @pl.when(i >= 2)
            def _():
                for a, way in parts:
                    ysend(i - 2, a, way).wait_send()

            hload(i).wait()
            for way in range(2):
                plain(i, way).wait_recv()
            for a in range(2):
                for way in range(2):
                    comb(i, way, a).wait_recv()

                def rows16(r, _, a=a):
                    for way in range(2):
                        at = pl.ds(pl.multiple_of(way * half + a * qt + r * 16, 16), 16)
                        y = hb[b, at, :].astype(F32) + (pb[4 * b + 3, at, :] + (fin[0, i, at, :] + fin[1, i, at, :]))
                        yb[b, at, :] = y.astype(BF16)
                    return 0

                lax.fori_loop(0, qt // 16, rows16, 0)
                for way in range(2):
                    ysend(i, a, way).start()

        def attend(g, head=True, tail=True):
            first, count = GROUPS[g]
            base, m = first * tt, count * tt
            nk = base + m
            t0 = nwp * g

            def norm(r, _):
                for a in range(4):
                    at = pl.ds(pl.multiple_of(r * 64 + a * 16, 16), 16)
                    y = yv[pl.ds(pl.multiple_of(base + r * 64 + a * 16, 16), 16), :].astype(F32)
                    xf = y * lax.rsqrt(jnp.mean(y * y, axis=-1, keepdims=True) + EPS) * nw[...]
                    xb[at, :] = xf.astype(BF16)
                return 0

            if head:
                for j in range(first, first + count):
                    for a, way in parts:
                        ysend(j, a, way).wait_recv()
                lax.fori_loop(0, m // 64, norm, 0)

            def heads(k, lo, hi, which=None):
                cl = [pl.ds(pl.multiple_of(k * WQ + a * HEAD, HEAD), HEAD) for a in range(lo, hi)]
                ss = [lax.dot_general(qb[0:m, cs], kv[0, 0:nk, cs], (((1,), (1,)), ((), ())), preferred_element_type=F32) for cs in cl]
                new = None if which is None else project(k + 1, which)
                keep = lax.broadcasted_iota(jnp.int32, (m, m), 0) >= lax.broadcasted_iota(jnp.int32, (m, m), 1)
                sm = []
                for sc in ss:
                    last = jnp.where(keep, sc[:, base:], -1e30)
                    sm.append(jnp.concatenate([sc[:, :base], last], axis=1) if base else last)
                mx = [jnp.max(sc, axis=-1, keepdims=True) for sc in sm]
                ps = [jnp.exp2((sc - mm) * SCALE2) for sc, mm in zip(sm, mx)]
                rs = [1.0 / jnp.sum(p, axis=-1, keepdims=True) for p in ps]
                pr = [(p * r).astype(BF16) for p, r in zip(ps, rs)]
                at = [jnp.dot(p, kv[1, 0:nk, cs], preferred_element_type=F32).astype(BF16) for p, cs in zip(pr, cl)]
                for v_, cs in zip(at, cl):
                    ab[0:m, cs] = v_
                return new

            def ready(k, which):
                wcopy(0, 0, t0 + 3 * k + which).wait()

            def project(k, which):
                w = wb[lax.rem(t0 + 3 * k + which, NW), 0:d, :]
                return jnp.dot(xb[0:m], w, preferred_element_type=F32).astype(BF16)

            def keepit(k, which, r):
                cols = pl.ds(pl.multiple_of(k * WQ, WQ), WQ)
                if which == 0:
                    qb[0:m, cols] = r
                else:
                    kv[which - 1, base:base + m, cols] = r
                wstart(t0 + 3 * k + which + NW)

            def both(k, _):
                for which in range(3):
                    ready(k, which)
                    lo, hi = which * NB // 2, min((which + 1) * NB // 2, NB)
                    r = heads(k - 1, lo, hi, which) if lo < hi else project(k, which)
                    keepit(k, which, r)
                return 0

            if head:
                for which in range(3):
                    ready(jnp.int32(0), which)
                    keepit(jnp.int32(0), which, project(jnp.int32(0), which))
                lax.fori_loop(1, nq, both, 0)
            if not tail:
                return

            heads(jnp.int32(nq - 1), 0, NB)
            if g >= 1:
                zcopy(g - 1).wait()

            def out(k, _):
                t = t0 + 3 * nq + k
                wcopy(3, 0, t).wait()
                r = jnp.dot(ab[0:m], wb[lax.rem(t, NW), :, 0:WZ], preferred_element_type=F32).astype(BF16)
                cols = pl.ds(pl.multiple_of(k * WZ, WZ), WZ)
                zb[0:m, cols] = (yv[base:base + m, cols].astype(F32) + r.astype(F32)).astype(BF16)
                wstart(t + NW)
                return 0

            lax.fori_loop(0, nz, out, 0)
            zcopy(g).start()

        parts = [(a, way) for a in range(2) for way in range(2)]

        def unit(u, gmc, gmn, bn, first=False):
            dst = lax.rem(u, 8)

            @pl.when(u + 1 < nu)
            def _():
                for cp in small(u + 1):
                    cp.wait()

            columns(u + 1, bn)

            @pl.when(u + 3 < nu)
            def _():
                for cp in small(u + 3):
                    cp.start()

            ng = tt // 16 // NP
            for k in range(NP):
                s = NP * u + k
                nxt = s + NS - 1

                @pl.when((nxt >= 4 * NP) & (nxt < nu * NP))
                def _(nxt=nxt):
                    for cp in panel(nxt):
                        cp.start()

                for cp in panel(s):
                    cp.wait()
                w = pan[lax.rem(s, NS)].reshape(kd, pw)
                acc = jnp.dot(gmc[...], w, preferred_element_type=F32)
                pb[dst, :, k * pw:(k + 1) * pw] = acc[0:tt] + (acc[tt:2 * tt] + acc[2 * tt:3 * tt])
                gates(gmn, ng * k, ng * (k + 1))
                early = s + 1 if first else nxt

                if not first or k < NP - 1:
                    @pl.when(early < 4 * NP)
                    def _(early=early):
                        exch(early).wait_recv()
                        for cp in panel(early):
                            cp.start()

        bar = pltpu.get_barrier_semaphore()
        for dev in (partner, right, left, ynext, yprev):
            pl.semaphore_signal(bar, inc=1, device_id=dev, device_id_type=MESH)
        pl.semaphore_wait(bar, 5)

        for s in range(4 * NP):
            exch(jnp.int32(s)).start()
        for u in range(2):
            for cp in small(u):
                cp.start()
        for t in range(NW):
            wstart(jnp.int32(t))
        for cp in small(0):
            cp.wait()
        columns(jnp.int32(0), 0)
        for cp in small(2):
            cp.start()
        hload(0).start()
        gates(gm0, 0, tt // 16)
        exch(jnp.int32(0)).wait_recv()
        for cp in panel(jnp.int32(0)):
            cp.start()

        unit(jnp.int32(0), gm0, gm1, 1, True)
        hop(jnp.int32(0), 0).start()
        hop(jnp.int32(0), 1).start()
        for s in range(NP, NS + 1):
            exch(jnp.int32(s)).wait_recv()
            for cp in panel(jnp.int32(s)):
                cp.start()

        def iteration(i, _):
            def two(v, _):
                u = 4 * i + 2 * v + 1
                @pl.when(v == 1)
                def _():
                    @pl.when(i >= 1)
                    def _():
                        finish(i - 1)

                    @pl.when(i + 1 < npair)
                    def _():
                        hload(i + 1).start()

                    for g, (first, count) in enumerate(GROUPS):
                        if first + count + 1 < npair:
                            @pl.when(i == first + count + 1)
                            def _(g=g):
                                attend(g)

                    for way in range(2):
                        hop(i, way).wait_recv()
                        src = 4 * lax.rem(i, 2) + 1 + way

                        def add(r, _, way=way, src=src):
                            at = pl.ds(pl.multiple_of(way * half + r * 16, 16), 16)
                            pb[src, at, :] = pb[src, at, :] + h1[way, i, pl.ds(pl.multiple_of(r * 16, 16), 16), :]
                            return 0

                        lax.fori_loop(0, half // 16, add, 0)
                        for a in range(2):
                            comb(i, way, a).start()

                    @pl.when(i >= 1)
                    def _():
                        for way in range(2):
                            hop(i - 1, way).wait_send()
                            plain(i - 1, way).wait_send()
                            for a in range(2):
                                comb(i - 1, way, a).wait_send()

                unit(u, gm1, gm0, 0)

                @pl.when(v == 0)
                def _():
                    plain(i, 0).start()

                @pl.when(u + 1 < nu)
                def _():
                    unit(u + 1, gm0, gm1, 1)

                    @pl.when(v == 0)
                    def _():
                        plain(i, 1).start()

                    @pl.when(v == 1)
                    def _():
                        hop(i + 1, 0).start()
                        hop(i + 1, 1).start()
                return 0

            lax.fori_loop(0, 2, two, 0)
            return 0

        lax.fori_loop(0, npair, iteration, 0)
        attend(2, tail=False)
        finish(jnp.int32(npair - 1))
        attend(2, head=False)
        attend(3)
        for s in range(4 * NP):
            exch(jnp.int32(s)).wait_send()
        for way in range(2):
            hop(npair - 1, way).wait_send()
            plain(npair - 1, way).wait_send()
            for a in range(2):
                comb(npair - 1, way, a).wait_send()
        for i in range(npair - 2, npair):
            for a, way in parts:
                ysend(i, a, way).wait_send()
        zcopy(len(GROUPS) - 1).wait()

    dma = pltpu.SemaphoreType.DMA
    anyspec = pl.BlockSpec(memory_space=pl.ANY)
    flops = 2 * 3 * 4 * ln * kd * d
    return pl.pallas_call(
        kernel,
        out_shape=(jax.ShapeDtypeStruct((ln, d), BF16), jax.ShapeDtypeStruct((4, el, capd, d), BF16)),
        in_specs=[anyspec] * 5 + [pl.BlockSpec(memory_space=pltpu.VMEM)] + [anyspec] * 4,
        out_specs=(anyspec, anyspec),
        scratch_shapes=[
            pltpu.VMEM((NS, ec, capd, pw), BF16),
            pltpu.VMEM((3 * tt, kd), BF16),
            pltpu.VMEM((3 * tt, kd), BF16),
            pltpu.VMEM((tt, kk), jnp.int32),
            pltpu.VMEM((tt, kk), F32),
            pltpu.VMEM((8, tt, d), F32),
            pltpu.VMEM((2, npair, half, d), F32),
            pltpu.VMEM((2, npair, tt, d), F32),
            pltpu.VMEM((2, kk, tt), jnp.int32),
            pltpu.VMEM((2, kk, tt), jnp.int32),
            pltpu.VMEM((2, kk, tt), F32),
            pltpu.VMEM((2, tt, d), BF16),
            pltpu.VMEM((2, tt, d), BF16),
            pltpu.VMEM((ln, d), BF16),
            pltpu.VMEM((mg, d), BF16),
            pltpu.VMEM((NW, hd, WQ), BF16),
            pltpu.VMEM((mg, hd), BF16),
            pltpu.VMEM((2, ln, hd), BF16),
            pltpu.VMEM((mg, hd), BF16),
            pltpu.VMEM((mg, d), BF16),
            dma((4 * NP,)), dma((4 * NP,)),
            dma((2, npair)), dma((2, npair)), dma((2, npair)), dma((2, npair)), dma((2, npair, 2)), dma((2, npair, 2)),
            dma((npair, 2, 2)), dma((npair, 2, 2)),
            dma((NS, 2)), dma((2, 3)), dma((2,)), dma((NW,)), dma,
        ],
        compiler_params=pltpu.CompilerParams(collective_id=1, has_side_effects=True, vmem_limit_bytes=67043328),
        cost_estimate=pl.CostEstimate(flops=flops, bytes_accessed=200 << 20, transcendentals=0),
        name='stage',
    )


def solution(mesh):
    n = mesh.shape['ep']
    npp = mesh.shape['pp']
    sp_o = P('pp', 'data', 'ep', None, None)
    sp_r = P('pp', 'data', None, None, None)
    sp_1 = P('pp', None)
    sp_w = P('pp', None, None)

    def body(o, idx, slot, gate, h, norm_w, wq, wk, wv, wo):
        _, nm, el, c, d = o.shape
        ln, kk = h.shape[3], idx.shape[4]
        hd = wq.shape[2]
        assert nm == 1 and h.shape[2] == 1
        stage = make_stage(n, npp, el, c, d, ln, kk, hd)
        turn = [jnp.swapaxes(a.reshape(n, ln, kk), 1, 2) for a in (idx, slot, gate)]
        z, _ = stage(o.reshape(el, c, d), *turn, h.reshape(ln, d), norm_w, wq[0], wk[0], wv[0], wo[0])
        return z.reshape(h.shape)

    return jax.shard_map(body, mesh=mesh, in_specs=(sp_o, sp_r, sp_r, sp_r, sp_o, sp_1, sp_w, sp_w, sp_w, sp_w), out_specs=sp_o, check_vma=False)
```

```python
import jax
import jax.numpy as jnp
from jax import lax
from jax.experimental import pallas as pl
from jax.experimental.pallas import tpu as pltpu
from jax.sharding import PartitionSpec as P

HEAD = 128
EPS = 1e-6
SCALE2 = HEAD ** -0.5 * 1.4426950408889634
MESH = pl.DeviceIdType.MESH
F32 = jnp.float32
BF16 = jnp.bfloat16
HALF = 64
NS = 3
NP = 2
NW = 3
NB = 4
GROUPS = ((0, 2), (2, 2), (4, 1), (5, 1))
WQ = 512
WZ = 256


def make_stage(n, npp, el, c, d, ln, kk, hd):
    nx = n // 2
    assert nx == 4
    capd = c // n
    ec = 2 * el
    kd = ec * capd
    tt = 2 * HALF
    npair = ln // tt
    nu = 4 * npair
    pw = d // NP
    half = HALF
    qt = half // 2
    nq = hd // WQ
    nz = d // WZ
    nwp = 3 * nq + nz
    assert WQ == NB * HEAD
    mg = tt * max(count for _, count in GROUPS)
    assert sum(count for _, count in GROUPS) == npair

    def kernel(o, idx, slot, gate, h, nw, wq, wk, wv, wo, z, ox,
               pan, gm0, gm1, colt, gatet, pb, h1, fin, ib, sb, gb, hb, yb, yv, xb, wb, qb, kv, ab, zb,
               xs, xr, h1s, h1r, pls, plr, cbs, cbr, ys, yr, psem, isem, hsem, wsem, zsem):
        ep = lax.axis_index('ep')
        pp = lax.axis_index('pp')
        core = lax.rem(ep, 2)
        x = ep // 2
        partner = {'ep': 2 * x + 1 - core}
        right = {'ep': 2 * lax.rem(x + 1, nx) + core}
        left = {'ep': 2 * lax.rem(x + nx - 1, nx) + core}
        ynext = {'pp': lax.rem(pp + 1, npp)}
        yprev = {'pp': lax.rem(pp + npp - 1, npp)}

        def remote(src, dst, ss, rs, dev):
            return pltpu.make_async_remote_copy(src_ref=src, dst_ref=dst, send_sem=ss, recv_sem=rs, device_id=dev, device_id_type=MESH)

        def owner(dp, cc):
            dd = jnp.where(dp == 0, 2, jnp.where(dp == 1, 1, jnp.where(dp == 2, 3, 0)))
            return 2 * lax.rem(x + dd, nx) + cc

        def exch(s):
            dp = s // NP
            q = owner(dp, 1 - core)
            cols = pl.ds(pl.multiple_of(lax.rem(s, NP) * pw, pw), pw)
            src = o.at[:, pl.ds(pl.multiple_of(q * capd, capd), capd), cols]
            return remote(src, ox.at[dp, :, :, cols], xs.at[s], xr.at[s], partner)

        def small(u):
            i = u // 4
            q = owner(lax.rem(u, 4), core)
            b = lax.rem(u, 2)
            cols = pl.ds(pl.multiple_of(i * tt, tt), tt)
            return [pltpu.make_async_copy(a.at[q, :, cols], v.at[b], isem.at[b, k])
                    for k, (a, v) in enumerate(((idx, ib), (slot, sb), (gate, gb)))]

        def panel(s):
            u = s // NP
            dp = lax.rem(u, 4)
            q = owner(dp, core)
            b = lax.rem(s, NS)
            cols = pl.ds(pl.multiple_of(lax.rem(s, NP) * pw, pw), pw)
            own = pltpu.make_async_copy(o.at[:, pl.ds(pl.multiple_of(q * capd, capd), capd), cols],
                                        pan.at[b, pl.ds(core * el, el)], psem.at[b, 0])
            oth = pltpu.make_async_copy(ox.at[dp, :, :, cols], pan.at[b, pl.ds((1 - core) * el, el)], psem.at[b, 1])
            return own, oth

        def hop(i, way):
            dev = right if way == 0 else left
            src = pb.at[4 * lax.rem(i, 2), pl.ds(way * half, half), :]
            return remote(src, h1.at[way, i], h1s.at[way, i], h1r.at[way, i], dev)

        def plain(i, way):
            dev = right if way == 0 else left
            at = pl.ds((1 - way) * half, half)
            src = pb.at[4 * lax.rem(i, 2) + 1 + way, at, :]
            return remote(src, fin.at[way, i, at, :], pls.at[way, i], plr.at[way, i], dev)

        def comb(i, way, a):
            dev = right if way == 0 else left
            at = pl.ds(way * half + a * qt, qt)
            src = pb.at[4 * lax.rem(i, 2) + 1 + way, at, :]
            return remote(src, fin.at[way, i, at, :], cbs.at[way, i, a], cbr.at[way, i, a], dev)

        def hload(i):
            b = lax.rem(i, 2)
            return pltpu.make_async_copy(h.at[pl.ds(pl.multiple_of(i * tt, tt), tt), :], hb.at[b], hsem.at[b])

        def ysend(i, a, way):
            at = way * half + a * qt
            rows = pl.ds(pl.multiple_of(i * tt + at, qt), qt)
            return remote(yb.at[lax.rem(i, 2), pl.ds(at, qt), :], yv.at[rows, :], ys.at[i, a, way], yr.at[i, a, way], ynext)

        def wcopy(which, k, t):
            b = lax.rem(t, NW)
            if which < 3:
                src = (wq, wk, wv)[which].at[:, pl.ds(pl.multiple_of(k * WQ, WQ), WQ)]
                return pltpu.make_async_copy(src, wb.at[b, pl.ds(0, d), :], wsem.at[b])
            src = wo.at[:, pl.ds(pl.multiple_of(k * WZ, WZ), WZ)]
            return pltpu.make_async_copy(src, wb.at[b, :, pl.ds(0, WZ)], wsem.at[b])

        def wstart(t):
            r = lax.rem(t, nwp)

            @pl.when(t < nwp * len(GROUPS))
            def _():
                for which in range(3):
                    @pl.when((r < 3 * nq) & (lax.rem(r, 3) == which))
                    def _(which=which):
                        wcopy(which, r // 3, t).start()

                @pl.when(r >= 3 * nq)
                def _():
                    wcopy(3, r - 3 * nq, t).start()

        def zcopy(g):
            first, count = GROUPS[g]
            return pltpu.make_async_copy(zb.at[pl.ds(0, count * tt), :], z.at[pl.ds(first * tt, count * tt), :], zsem)

        def columns(u, b):
            q = owner(lax.rem(u, 4), core)
            e = ib[b] - x * ec
            ss = sb[b]
            ok = (e >= 0) & (e < ec) & (ss >= 0)
            col = jnp.where(ok, e * capd + (ss - q * capd), -1)
            colt[...] = col.T
            gatet[...] = gb[b].T

        def gates(gm, g0, g1):
            for g in range(g0, g1):
                rows = pl.ds(16 * g, 16)
                col = colt[rows, :].astype(jnp.int16)
                gg = gatet[rows, :]
                hi = gg.astype(BF16)
                r = gg - hi.astype(F32)
                mi = r.astype(BF16)
                lw = (r - mi.astype(F32)).astype(BF16)
                cs = [jnp.broadcast_to(col[:, j:j + 1], (16, 128)) for j in range(kk)]
                ws = [[jnp.broadcast_to(p[:, j:j + 1], (16, 128)) for j in range(kk)] for p in (hi, mi, lw)]
                io = lax.broadcasted_iota(jnp.int16, (16, 128), 1)
                for v in range(kd // 128):
                    at = io + jnp.int16(128 * v)
                    t = [jnp.zeros((16, 128), BF16) for _ in range(3)]
                    for j in range(kk):
                        m = cs[j] == at
                        for k in range(3):
                            t[k] = jnp.where(m, ws[k][j], t[k])
                    for k in range(3):
                        gm[k * tt + 16 * g:k * tt + 16 * g + 16, 128 * v:128 * v + 128] = t[k]

        def finish(i):
            b = lax.rem(i, 2)

            @pl.when(i >= 2)
            def _():
                for a, way in parts:
                    ysend(i - 2, a, way).wait_send()

            hload(i).wait()
            for way in range(2):
                plain(i, way).wait_recv()
            for a in range(2):
                for way in range(2):
                    comb(i, way, a).wait_recv()

                def rows16(r, _, a=a):
                    for way in range(2):
                        at = pl.ds(pl.multiple_of(way * half + a * qt + r * 16, 16), 16)
                        y = hb[b, at, :].astype(F32) + (pb[4 * b + 3, at, :] + (fin[0, i, at, :] + fin[1, i, at, :]))
                        yb[b, at, :] = y.astype(BF16)
                    return 0

                lax.fori_loop(0, qt // 16, rows16, 0)
                for way in range(2):
                    ysend(i, a, way).start()

        def attend(g, head=True, tail=True):
            first, count = GROUPS[g]
            base, m = first * tt, count * tt
            nk = base + m
            t0 = nwp * g

            def norm(r, _):
                for a in range(4):
                    at = pl.ds(pl.multiple_of(r * 64 + a * 16, 16), 16)
                    y = yv[pl.ds(pl.multiple_of(base + r * 64 + a * 16, 16), 16), :].astype(F32)
                    xf = y * lax.rsqrt(jnp.mean(y * y, axis=-1, keepdims=True) + EPS) * nw[...]
                    xb[at, :] = xf.astype(BF16)
                return 0

            if head:
                for j in range(first, first + count):
                    for a, way in parts:
                        ysend(j, a, way).wait_recv()
                lax.fori_loop(0, m // 64, norm, 0)

            def heads(k, lo, hi, which=None):
                cl = [pl.ds(pl.multiple_of(k * WQ + a * HEAD, HEAD), HEAD) for a in range(lo, hi)]
                ss = [lax.dot_general(qb[0:m, cs], kv[0, 0:nk, cs], (((1,), (1,)), ((), ())), preferred_element_type=F32) for cs in cl]
                new = None if which is None else project(k + 1, which)
                keep = lax.broadcasted_iota(jnp.int32, (m, m), 0) >= lax.broadcasted_iota(jnp.int32, (m, m), 1)
                sm = []
                for sc in ss:
                    last = jnp.where(keep, sc[:, base:], -1e30)
                    sm.append(jnp.concatenate([sc[:, :base], last], axis=1) if base else last)
                mx = [jnp.max(sc, axis=-1, keepdims=True) for sc in sm]
                ps = [jnp.exp2((sc - mm) * SCALE2) for sc, mm in zip(sm, mx)]
                rs = [1.0 / jnp.sum(p, axis=-1, keepdims=True) for p in ps]
                pr = [(p * r).astype(BF16) for p, r in zip(ps, rs)]
                at = [jnp.dot(p, kv[1, 0:nk, cs], preferred_element_type=F32).astype(BF16) for p, cs in zip(pr, cl)]
                for v_, cs in zip(at, cl):
                    ab[0:m, cs] = v_
                return new

            def ready(k, which):
                wcopy(0, 0, t0 + 3 * k + which).wait()

            def project(k, which):
                w = wb[lax.rem(t0 + 3 * k + which, NW), 0:d, :]
                return jnp.dot(xb[0:m], w, preferred_element_type=F32).astype(BF16)

            def keepit(k, which, r):
                cols = pl.ds(pl.multiple_of(k * WQ, WQ), WQ)
                if which == 0:
                    qb[0:m, cols] = r
                else:
                    kv[which - 1, base:base + m, cols] = r
                wstart(t0 + 3 * k + which + NW)

            def both(k, _):
                for which in range(3):
                    ready(k, which)
                    lo, hi = which * NB // 2, min((which + 1) * NB // 2, NB)
                    r = heads(k - 1, lo, hi, which) if lo < hi else project(k, which)
                    keepit(k, which, r)
                return 0

            if head:
                for which in range(3):
                    ready(jnp.int32(0), which)
                    keepit(jnp.int32(0), which, project(jnp.int32(0), which))
                lax.fori_loop(1, nq, both, 0)
            if not tail:
                return

            heads(jnp.int32(nq - 1), 0, NB)
            if g >= 1:
                zcopy(g - 1).wait()

            def out(k, _):
                t = t0 + 3 * nq + k
                wcopy(3, 0, t).wait()
                r = jnp.dot(ab[0:m], wb[lax.rem(t, NW), :, 0:WZ], preferred_element_type=F32).astype(BF16)
                cols = pl.ds(pl.multiple_of(k * WZ, WZ), WZ)
                zb[0:m, cols] = (yv[base:base + m, cols].astype(F32) + r.astype(F32)).astype(BF16)
                wstart(t + NW)
                return 0

            lax.fori_loop(0, nz, out, 0)
            zcopy(g).start()

        parts = [(a, way) for a in range(2) for way in range(2)]

        def unit(u, gmc, gmn, bn, first=False):
            dst = lax.rem(u, 8)

            @pl.when(u + 1 < nu)
            def _():
                for cp in small(u + 1):
                    cp.wait()

            columns(u + 1, bn)

            @pl.when(u + 3 < nu)
            def _():
                for cp in small(u + 3):
                    cp.start()

            ng = tt // 16 // NP
            for k in range(NP):
                s = NP * u + k
                nxt = s + NS - 1

                @pl.when((nxt >= 4 * NP) & (nxt < nu * NP))
                def _(nxt=nxt):
                    for cp in panel(nxt):
                        cp.start()

                for cp in panel(s):
                    cp.wait()
                w = pan[lax.rem(s, NS)].reshape(kd, pw)
                acc = jnp.dot(gmc[...], w, preferred_element_type=F32)
                pb[dst, :, k * pw:(k + 1) * pw] = acc[0:tt] + (acc[tt:2 * tt] + acc[2 * tt:3 * tt])
                gates(gmn, ng * k, ng * (k + 1))
                early = s + 1 if first else nxt

                if not first or k < NP - 1:
                    @pl.when(early < 4 * NP)
                    def _(early=early):
                        exch(early).wait_recv()

                        @pl.when(early + 2 < 4 * NP)
                        def _():
                            exch(early + 2).start()

                        for cp in panel(early):
                            cp.start()

        bar = pltpu.get_barrier_semaphore()
        for dev in (partner, right, left, ynext, yprev):
            pl.semaphore_signal(bar, inc=1, device_id=dev, device_id_type=MESH)
        pl.semaphore_wait(bar, 5)

        for s in range(2):
            exch(jnp.int32(s)).start()
        for u in range(2):
            for cp in small(u):
                cp.start()
        for t in range(NW):
            wstart(jnp.int32(t))
        for cp in small(0):
            cp.wait()
        columns(jnp.int32(0), 0)
        for cp in small(2):
            cp.start()
        hload(0).start()
        gates(gm0, 0, tt // 16)
        exch(jnp.int32(0)).wait_recv()
        exch(jnp.int32(2)).start()
        for cp in panel(jnp.int32(0)):
            cp.start()

        unit(jnp.int32(0), gm0, gm1, 1, True)
        hop(jnp.int32(0), 0).start()
        hop(jnp.int32(0), 1).start()
        for s in range(NP, NS + 1):
            exch(jnp.int32(s)).wait_recv()
            exch(jnp.int32(s + 2)).start()
            for cp in panel(jnp.int32(s)):
                cp.start()

        def iteration(i, _):
            def two(v, _):
                u = 4 * i + 2 * v + 1
                @pl.when(v == 1)
                def _():
                    @pl.when(i >= 1)
                    def _():
                        finish(i - 1)

                    @pl.when(i + 1 < npair)
                    def _():
                        hload(i + 1).start()

                    for g, (first, count) in enumerate(GROUPS):
                        if first + count + 1 < npair:
                            @pl.when(i == first + count + 1)
                            def _(g=g):
                                attend(g)

                    for way in range(2):
                        hop(i, way).wait_recv()
                        src = 4 * lax.rem(i, 2) + 1 + way

                        def add(r, _, way=way, src=src):
                            at = pl.ds(pl.multiple_of(way * half + r * 16, 16), 16)
                            pb[src, at, :] = pb[src, at, :] + h1[way, i, pl.ds(pl.multiple_of(r * 16, 16), 16), :]
                            return 0

                        lax.fori_loop(0, half // 16, add, 0)
                        for a in range(2):
                            comb(i, way, a).start()

                    @pl.when(i >= 1)
                    def _():
                        for way in range(2):
                            hop(i - 1, way).wait_send()
                            plain(i - 1, way).wait_send()
                            for a in range(2):
                                comb(i - 1, way, a).wait_send()

                unit(u, gm1, gm0, 0)

                @pl.when(v == 0)
                def _():
                    plain(i, 0).start()

                @pl.when(u + 1 < nu)
                def _():
                    unit(u + 1, gm0, gm1, 1)

                    @pl.when(v == 0)
                    def _():
                        plain(i, 1).start()

                    @pl.when(v == 1)
                    def _():
                        hop(i + 1, 0).start()
                        hop(i + 1, 1).start()
                return 0

            lax.fori_loop(0, 2, two, 0)
            return 0

        lax.fori_loop(0, npair, iteration, 0)
        attend(2, tail=False)
        finish(jnp.int32(npair - 1))
        attend(2, head=False)
        attend(3)
        for s in range(4 * NP):
            exch(jnp.int32(s)).wait_send()
        for way in range(2):
            hop(npair - 1, way).wait_send()
            plain(npair - 1, way).wait_send()
            for a in range(2):
                comb(npair - 1, way, a).wait_send()
        for i in range(npair - 2, npair):
            for a, way in parts:
                ysend(i, a, way).wait_send()
        zcopy(len(GROUPS) - 1).wait()

    dma = pltpu.SemaphoreType.DMA
    anyspec = pl.BlockSpec(memory_space=pl.ANY)
    flops = 2 * 3 * 4 * ln * kd * d
    return pl.pallas_call(
        kernel,
        out_shape=(jax.ShapeDtypeStruct((ln, d), BF16), jax.ShapeDtypeStruct((4, el, capd, d), BF16)),
        in_specs=[anyspec] * 5 + [pl.BlockSpec(memory_space=pltpu.VMEM)] + [anyspec] * 4,
        out_specs=(anyspec, anyspec),
        scratch_shapes=[
            pltpu.VMEM((NS, ec, capd, pw), BF16),
            pltpu.VMEM((3 * tt, kd), BF16),
            pltpu.VMEM((3 * tt, kd), BF16),
            pltpu.VMEM((tt, kk), jnp.int32),
            pltpu.VMEM((tt, kk), F32),
            pltpu.VMEM((8, tt, d), F32),
            pltpu.VMEM((2, npair, half, d), F32),
            pltpu.VMEM((2, npair, tt, d), F32),
            pltpu.VMEM((2, kk, tt), jnp.int32),
            pltpu.VMEM((2, kk, tt), jnp.int32),
            pltpu.VMEM((2, kk, tt), F32),
            pltpu.VMEM((2, tt, d), BF16),
            pltpu.VMEM((2, tt, d), BF16),
            pltpu.VMEM((ln, d), BF16),
            pltpu.VMEM((mg, d), BF16),
            pltpu.VMEM((NW, hd, WQ), BF16),
            pltpu.VMEM((mg, hd), BF16),
            pltpu.VMEM((2, ln, hd), BF16),
            pltpu.VMEM((mg, hd), BF16),
            pltpu.VMEM((mg, d), BF16),
            dma((4 * NP,)), dma((4 * NP,)),
            dma((2, npair)), dma((2, npair)), dma((2, npair)), dma((2, npair)), dma((2, npair, 2)), dma((2, npair, 2)),
            dma((npair, 2, 2)), dma((npair, 2, 2)),
            dma((NS, 2)), dma((2, 3)), dma((2,)), dma((NW,)), dma,
        ],
        compiler_params=pltpu.CompilerParams(collective_id=1, has_side_effects=True, vmem_limit_bytes=67043328),
        cost_estimate=pl.CostEstimate(flops=flops, bytes_accessed=200 << 20, transcendentals=0),
        name='stage',
    )


def solution(mesh):
    n = mesh.shape['ep']
    npp = mesh.shape['pp']
    sp_o = P('pp', 'data', 'ep', None, None)
    sp_r = P('pp', 'data', None, None, None)
    sp_1 = P('pp', None)
    sp_w = P('pp', None, None)

    def body(o, idx, slot, gate, h, norm_w, wq, wk, wv, wo):
        _, nm, el, c, d = o.shape
        ln, kk = h.shape[3], idx.shape[4]
        hd = wq.shape[2]
        assert nm == 1 and h.shape[2] == 1
        stage = make_stage(n, npp, el, c, d, ln, kk, hd)
        turn = [jnp.swapaxes(a.reshape(n, ln, kk), 1, 2) for a in (idx, slot, gate)]
        z, _ = stage(o.reshape(el, c, d), *turn, h.reshape(ln, d), norm_w, wq[0], wk[0], wv[0], wo[0])
        return z.reshape(h.shape)

    return jax.shard_map(body, mesh=mesh, in_specs=(sp_o, sp_r, sp_r, sp_r, sp_o, sp_1, sp_w, sp_w, sp_w, sp_w), out_specs=sp_o, check_vma=False)
```
